32 devices in a mesh: wide: 8 (over z, y), narrow: 4 (over x, core).
Axes of the slice: x: 2, y: 2, z: 4, core: 2. Of those that a mesh axis runs over, the one named last changes fastest.
Arguments:
- queries: bfloat16 [2048, 1024], P(('wide', 'narrow')), may hold values from -16 to 16
- documents: bfloat16 [2048, 1024], P(('wide', 'narrow')), may hold values from -16 to 16
- user_ids: int32 [2048], replicated, may hold values from 0 to 1663, as said below
Outputs:
- query_grad: bfloat16 [2048, 1024], P(('wide', 'narrow'))
- doc_grad: bfloat16 [2048, 1024], P(('wide', 'narrow'))
- loss: float32 [], replicated
The draws below stay inside these ranges and needn't reach their ends.
Inputs may be any that keep to these rules, and one draw needn't show every extreme that they name: `user_ids`: each user id names at most 4 rows; rows with a common id lie in the same quarter of the 2048 rows.
All inputs are finite; a program needn't handle non-finite values.
Results may differ from the reference program's by a relative error of at most 0.004.
The reference program's roundings to bfloat16 on the way (of `weights`) count: a program that leaves them out, or rounds other values in their place, can miss the bound.
Values may be sent and summed in bfloat16 or wider, within the bound.
No kernel may reach another device: no remote copies, remote signals or barrier semaphores. Data moves between devices by JAX's collectives and lax.ppermute only.
A program may use at most 64 MiB of HBM per device.

```python
import math
import jax
import jax.numpy as jnp
from jax import lax

D = 1024
BATCH = 2048


def draw_pair(key):
    query_key = jax.random.fold_in(key, 11)
    doc_key = jax.random.fold_in(key, 12)
    query_raw = jnp.clip(jax.random.normal(query_key, (BATCH, D), jnp.float32), -4.0, 4.0)
    doc_raw = jnp.clip(jax.random.normal(doc_key, (BATCH, D), jnp.float32), -4.0, 4.0)
    return (query_raw, doc_raw)


def draw_queries(key, part):
    return draw_pair(key)[0].astype(jnp.bfloat16)


def draw_documents(key, part):
    return draw_pair(key)[1].astype(jnp.bfloat16)


def draw_user_ids(key, part):
    quarter = BATCH // 4
    pieces = []
    for band in range(4):
        order = jax.random.permutation(jax.random.fold_in(key, 21 + band), jnp.arange(quarter, dtype=jnp.int32))
        pieces.append(band * quarter + order // (band + 1))
    return jnp.concatenate(pieces).astype(jnp.int32)


def setup_inputs(seed: int = 0) -> dict:
    splits = jax.random.split(jax.random.key(seed), 4)
    return {
        "queries": draw_queries(jax.random.fold_in(splits[3], 71), 0),
        "documents": draw_documents(jax.random.fold_in(splits[3], 71), 0),
        "user_ids": draw_user_ids(jax.random.fold_in(splits[3], 71), 0),
    }


def reference(queries, documents, user_ids):
    score_scale = 3.0 / math.sqrt(D)
    block = math.gcd(BATCH, 512)
    blocks = BATCH // block
    query_blocks = queries.reshape(blocks, block, D)
    user_blocks = user_ids.reshape(blocks, block)

    def block_scores(query_rows):
        product = lax.dot_general(query_rows, documents, (((1,), (1,)), ((), ())), preferred_element_type=jnp.float32)
        return product * score_scale

    def statistics(inputs):
        query_rows, users = inputs
        scores = block_scores(query_rows)
        peak = lax.optimization_barrier(jnp.max(scores, axis=1))
        log_denom = peak + jnp.log(lax.optimization_barrier(jnp.sum(jnp.exp(scores - peak[:, None]), axis=1)))
        positive = users[:, None] == user_ids[None, :]
        counts = lax.optimization_barrier(jnp.sum(positive.astype(jnp.float32), axis=1))
        pos_sum = lax.optimization_barrier(jnp.sum(jnp.where(positive, scores, jnp.float32(0.0)), axis=1))
        return (log_denom, counts, pos_sum)
    log_denom, counts, pos_sum = lax.map(statistics, (query_blocks, user_blocks))
    total = jnp.sum(counts)
    loss = jnp.sum(counts * log_denom - pos_sum) / total

    def backward(doc_accum, inputs):
        query_rows, users, block_denom, block_counts = inputs
        scores = block_scores(query_rows)
        positive = (users[:, None] == user_ids[None, :]).astype(jnp.float32)
        probs = jnp.exp(scores - block_denom[:, None])
        weights = (jnp.float32(BATCH) * (block_counts[:, None] * probs - positive) / total).astype(jnp.bfloat16)
        query_part = jnp.dot(weights, documents, preferred_element_type=jnp.float32) * score_scale
        doc_part = lax.dot_general(weights, query_rows, (((0,), (0,)), ((), ())), preferred_element_type=jnp.float32) * score_scale
        return (doc_accum + doc_part, query_part.astype(jnp.bfloat16))
    doc_accum, query_parts = lax.scan(backward, jnp.zeros((BATCH, D), jnp.float32), (query_blocks, user_blocks, log_denom, counts))
    return (query_parts.reshape(BATCH, D), doc_accum.astype(jnp.bfloat16), loss)
```

```python
import math

import jax
import jax.numpy as jnp
from jax import lax
from jax.sharding import Mesh, PartitionSpec as P


QUARTERS = 4
ALL = ("quarter", "lane", "chip", "core")
PLANE = ("lane", "chip")
DIRECT = 8


def flat_index(axes):
    return lax.axis_index(axes)


def send_pieces(pieces, axes):
    count = len(pieces)
    if count <= DIRECT:
        out = [pieces[0]] + [None] * (count - 1)
        for k in range(count - 1, 0, -1):
            out[k] = lax.ppermute(pieces[k], axes, [(i, i ^ k) for i in range(count)])
        return out
    order = jnp.bitwise_xor(flat_index(axes), jnp.arange(count))
    placed = jnp.take(jnp.stack(pieces), order, axis=0)
    moved = jnp.take(lax.all_to_all(placed, axes, 0, 0, tiled=True), order, axis=0)
    return [pieces[0]] + [moved[k] for k in range(1, count)]


def swap_cores(array):
    return lax.ppermute(array, "core", [(0, 1), (1, 0)])


def local(queries, documents, user_ids):
    rows, width = queries.shape
    quarters = lax.axis_size("quarter")
    plane = lax.axis_size("lane") * lax.axis_size("chip")
    devices = quarters * plane * 2
    batch_rows = jnp.float32(devices * rows)
    score_scale = 3.0 / math.sqrt(width)
    my_quarter = lax.axis_index("quarter")
    my_plane = flat_index(PLANE)
    my_core = lax.axis_index("core")

    q_parts = send_pieces([queries] * quarters, "quarter")
    d_parts = send_pieces([documents] * plane, PLANE)
    d_mine = jnp.concatenate(d_parts, 0)
    d_other = swap_cores(d_mine)
    q_mine = jnp.concatenate(q_parts, 0)
    docs = jnp.concatenate([d_mine, d_other], 0)

    table = user_ids.reshape(quarters, plane, 2, rows)
    quarter_ids = user_ids.reshape(quarters, plane * 2 * rows)
    total = jnp.sum((quarter_ids[:, :, None] == quarter_ids[:, None, :]).astype(jnp.float32))
    q_order = jnp.bitwise_xor(my_quarter, jnp.arange(quarters))
    q_ids = lax.dynamic_index_in_dim(
        lax.dynamic_index_in_dim(table, my_plane, 1, False), my_core, 1, False
    )
    row_counts = jnp.sum((q_ids[:, :, None] == quarter_ids[:, None, :]).astype(jnp.float32), 2)
    counts = jnp.take(row_counts, q_order, axis=0).reshape(1, -1)
    d_order = jnp.bitwise_xor(my_plane, jnp.arange(plane))
    plane_table = jnp.take(lax.dynamic_index_in_dim(table, my_quarter, 0, False), d_order, axis=0)
    d_ids = jnp.concatenate(
        [
            lax.dynamic_index_in_dim(plane_table, my_core, 1, False).reshape(-1),
            lax.dynamic_index_in_dim(plane_table, 1 - my_core, 1, False).reshape(-1),
        ]
    )
    own_ids = lax.dynamic_index_in_dim(q_ids, my_quarter, 0, False)
    positive = d_ids[:, None] == own_ids[None, :]

    contract = lambda a, b, da, db: lax.dot_general(
        a, b, (((da,), (db,)), ((), ())), preferred_element_type=jnp.float32
    )
    scores = contract(docs, q_mine, 1, 1) * score_scale
    peak = jnp.max(scores, 0, keepdims=True)
    lse = peak + jnp.log(jnp.sum(jnp.exp(scores - peak), 0, keepdims=True))
    q_other = swap_cores(q_mine)
    lses = send_pieces([lse] * quarters, "quarter")
    lses = [part.reshape(quarters, rows) for part in lses]
    aligned = jnp.stack(
        [jnp.stack([lses[j][k ^ j] for k in range(quarters)]) for j in range(quarters)]
    )
    log_denom = jax.nn.logsumexp(aligned, axis=0).reshape(1, -1)
    pos_all = jnp.concatenate(
        [positive.astype(jnp.float32), jnp.zeros((positive.shape[0], (quarters - 1) * rows), jnp.float32)], 1
    )
    weights = (batch_rows * (counts * jnp.exp(scores - log_denom) - pos_all) / total).astype(jnp.bfloat16)

    half = plane * rows
    w_in = swap_cores(weights[half:])
    q_share = [
        contract(weights[:, k * rows : (k + 1) * rows], docs, 0, 0) * score_scale
        for k in range(quarters)
    ]
    q_got = send_pieces([part.astype(jnp.bfloat16) for part in q_share], "quarter")
    query_grad = q_share[0] + sum(part.astype(jnp.float32) for part in q_got[1:])
    d_share = [
        (
            contract(weights[k * rows : (k + 1) * rows], q_mine, 1, 0)
            + contract(w_in[k * rows : (k + 1) * rows], q_other, 1, 0)
        )
        * score_scale
        for k in range(plane)
    ]
    d_got = send_pieces([part.astype(jnp.bfloat16) for part in d_share], PLANE)
    doc_grad = d_share[0] + sum(part.astype(jnp.float32) for part in d_got[1:])

    row_loss = jnp.sum(counts[:, :rows] * log_denom[:, :rows]) - jnp.sum(
        jnp.where(positive, scores[:, :rows], 0.0)
    )
    spread = jnp.broadcast_to(row_loss, (devices, 128))
    loss = jnp.sum(lax.all_to_all(spread, ALL, 0, 0, tiled=True)[:, 0]) / total
    return query_grad.astype(jnp.bfloat16), doc_grad.astype(jnp.bfloat16), loss


def solution(mesh):
    wide, narrow = mesh.shape["wide"], mesh.shape["narrow"]
    grid = Mesh(
        mesh.devices.reshape(QUARTERS, wide // QUARTERS, narrow // 2, 2), ALL
    )
    return jax.shard_map(
        local,
        mesh=grid,
        in_specs=(P(ALL, None), P(ALL, None), P()),
        out_specs=(P(ALL, None), P(ALL, None), P()),
        check_vma=False,
    )
```

```python
import functools
import math

import jax
import jax.numpy as jnp
from jax import lax
from jax.experimental import pallas as pl
from jax.experimental.pallas import tpu as pltpu
from jax.sharding import Mesh, PartitionSpec as P


QUARTERS = 4
ALL = ("quarter", "lane", "chip", "core")
PLANE = ("lane", "chip")
DIRECT = 8
CHUNK = 256
F32, BF16 = jnp.float32, jnp.bfloat16


def send_pieces(pieces, axes):
    count = len(pieces)
    if count <= DIRECT:
        out = [pieces[0]] + [None] * (count - 1)
        for k in range(count - 1, 0, -1):
            out[k] = lax.ppermute(pieces[k], axes, [(i, i ^ k) for i in range(count)])
        return out
    order = jnp.bitwise_xor(lax.axis_index(axes), jnp.arange(count))
    placed = jnp.take(jnp.stack(pieces), order, axis=0)
    moved = jnp.take(lax.all_to_all(placed, axes, 0, 0, tiled=True), order, axis=0)
    return [pieces[0]] + [moved[k] for k in range(1, count)]


def swap_cores(array):
    return lax.ppermute(array, "core", [(0, 1), (1, 0)])


def tree_sum(terms):
    while len(terms) > 1:
        terms = [terms[i] + terms[i + 1] for i in range(0, len(terms), 2)]
    return terms[0]


def contract(a, b, da, db):
    return lax.dot_general(a, b, (((da,), (db,)), ((), ())), preferred_element_type=F32)


def call(kernel, outs, *args):
    vmem = pl.BlockSpec(memory_space=pltpu.VMEM)
    return pl.pallas_call(
        kernel,
        out_shape=[jax.ShapeDtypeStruct(shape, dtype) for shape, dtype in outs],
        in_specs=[vmem] * len(args),
        out_specs=[vmem] * len(outs),
    )(*args)


def each_chunk(total, body):
    if total <= 2 * CHUNK:
        for i in range(total // CHUNK):
            body(i * CHUNK)
    else:

        @pl.loop(0, total // CHUNK)
        def _(i):
            body(pl.multiple_of(i * CHUNK, CHUNK))


def score_kernel(scale, rows, docs, queries, positive, scores, stats):
    count = docs.shape[0]
    cols = queries.shape[0]
    peak = jnp.full((1, cols), -jnp.inf, F32)
    pos = jnp.zeros((1, rows), F32)
    stats[...] = jnp.zeros(stats.shape, F32)
    stats[0:1, :cols] = peak
    queries_now = queries[...]

    def first(at):
        part = contract(docs[pl.ds(at, CHUNK), :], queries_now, 1, 1) * scale
        scores[pl.ds(at, CHUNK), :] = part
        stats[0:1, :cols] = jnp.maximum(stats[0:1, :cols], jnp.max(part, 0, keepdims=True))
        chosen = jnp.where(positive[pl.ds(at, CHUNK), :] > 0.0, part[:, :rows], 0.0)
        stats[1:2, :rows] += jnp.sum(chosen, 0, keepdims=True)

    each_chunk(count, first)
    peak = stats[0:1, :cols]

    def second(at):
        stats[2:3, :cols] += jnp.sum(jnp.exp(scores[pl.ds(at, CHUNK), :] - peak), 0, keepdims=True)

    each_chunk(count, second)
    stats[0:1, :cols] = peak + jnp.log(stats[2:3, :cols])


def share_kernel(scale, rows, scores, stats, docs, *outs):
    cols = scores.shape[1]
    lse = stats[0:1, :cols]
    total = None
    for at in range(0, scores.shape[0], 2 * CHUNK):
        probs = jnp.exp(scores[at : at + 2 * CHUNK, :] - lse)
        part = contract(jnp.transpose(probs)[rows:].astype(BF16), docs[at : at + 2 * CHUNK, :], 1, 0)
        total = part if total is None else total + part
    total = (total * scale).astype(BF16)
    for k, out in enumerate(outs):
        out[...] = total[k * rows : (k + 1) * rows]


def weight_kernel(batch_rows, rows, scores, s0, s1, s2, s3, counts, total, positive, *outs):
    w_mine, w_send, gains, loss = outs
    cols = scores.shape[1]
    half = scores.shape[0] // 2
    stats = [s[...] for s in (s0, s1, s2, s3)]
    rest = cols // rows
    lses = [
        jnp.concatenate([s[0:1, (k ^ j) * rows : (k ^ j) * rows + rows] for k in range(rest)], 1)
        for j, s in enumerate(stats)
    ]
    top = functools.reduce(jnp.maximum, lses)
    log_denom = top + jnp.log(tree_sum([jnp.exp(a - top) for a in lses]))
    row_counts = counts[...]
    all_pairs = total[...]

    def fill(out, base):
        def body(at):
            src = pl.ds(base + at, CHUNK)
            raw = row_counts * jnp.exp(scores[src, :] - log_denom)
            own = raw[:, : 2 * rows]
            pad = jnp.concatenate([positive[src, :], jnp.zeros((CHUNK, rows), F32)], 1)
            raw = jnp.concatenate([own - pad, raw[:, 2 * rows :]], 1)
            out[pl.ds(at, CHUNK), :] = (batch_rows * raw / all_pairs).astype(BF16)

        each_chunk(half, body)

    fill(w_send, half)
    fill(w_mine, 0)
    factor = batch_rows * row_counts[:, :rows] / all_pairs[:, :rows]
    lanes = [factor * jnp.exp(a[:, :rows] - log_denom[:, :rows]) for a in lses]
    tall = jnp.concatenate(lanes + lanes, 0)
    gains[...] = jnp.transpose(jnp.concatenate([tall, tall], 1))[:rows]
    terms = row_counts * log_denom
    line = tree_sum(
        [
            jnp.sum(terms[:, k * rows : (k + 1) * rows] - stats[k][1:2, :rows], 1, keepdims=True)
            for k in range(rest)
        ]
    )
    loss[...] = jnp.broadcast_to(line, loss.shape)


def own_kernel(scale, w_mine, w_send, docs, out):
    half = w_mine.shape[0]
    rows = out.shape[0]
    total = None
    for base, ref in ((0, w_mine), (half, w_send)):
        for at in range(0, half, CHUNK):
            w = jnp.transpose(ref[at : at + CHUNK, :].astype(F32))[:rows].astype(BF16)
            part = contract(w, docs[base + at : base + at + CHUNK, :], 1, 0)
            total = part if total is None else total + part
    out[...] = total * scale


def doc_kernel(scale, rows, w_mine, w_in, q_mine, q_other, own, *outs):
    half = w_mine.shape[0]

    def body(at):
        part = contract(w_mine[pl.ds(at, CHUNK), :], q_mine[...], 1, 0)
        part = (part + contract(w_in[pl.ds(at, CHUNK), :], q_other[...], 1, 0)) * scale
        if len(outs) == 1 or half != CHUNK:
            outs[0][pl.ds(at, CHUNK), :] = part.astype(BF16)
            return part
        own[...] = part[:rows]
        for k, out in enumerate(outs, 1):
            out[...] = part[k * rows : (k + 1) * rows].astype(BF16)
        return part

    if half == CHUNK:
        body(0)
    else:
        own[...] = body(0)[:rows]

        @pl.loop(1, half // CHUNK)
        def _(i):
            body(pl.multiple_of(i * CHUNK, CHUNK))


def query_sum_kernel(own, gains, *refs):
    *got, out = refs
    total = own[...]
    for k, ref in enumerate(got, 1):
        total = total + gains[:, k : k + 1] * ref[...].astype(F32)
    out[...] = total.astype(BF16)


def doc_sum_kernel(own, *refs):
    *got, out = refs
    total = own[...]
    for ref in got:
        total = total + ref[...].astype(F32)
    out[...] = total.astype(BF16)


def local(queries, documents, user_ids):
    rows, width = queries.shape
    quarters = lax.axis_size("quarter")
    plane = lax.axis_size("lane") * lax.axis_size("chip")
    devices = quarters * plane * 2
    batch_rows = float(devices * rows)
    scale = 3.0 / math.sqrt(width)
    my_quarter = lax.axis_index("quarter")
    my_plane = lax.axis_index(PLANE)
    my_core = lax.axis_index("core")
    cols = quarters * rows
    half = plane * rows
    piece = ((rows, width), BF16)

    d_parts = send_pieces([documents] * plane, PLANE)
    q_parts = send_pieces([queries] * quarters, "quarter")
    d_mine = jnp.concatenate(d_parts, 0)
    d_other = swap_cores(d_mine)
    q_mine = jnp.concatenate(q_parts, 0)
    docs = jnp.concatenate([d_mine, d_other], 0)

    table = user_ids.reshape(quarters, plane, 2, rows)
    quarter_ids = user_ids.reshape(quarters, plane * 2 * rows)
    total = jnp.sum((quarter_ids[:, :, None] == quarter_ids[:, None, :]).astype(F32))
    total = jnp.broadcast_to(total, (1, cols))
    q_order = jnp.bitwise_xor(my_quarter, jnp.arange(quarters))
    q_ids = lax.dynamic_index_in_dim(
        lax.dynamic_index_in_dim(table, my_plane, 1, False), my_core, 1, False
    )
    row_counts = jnp.sum((q_ids[:, :, None] == quarter_ids[:, None, :]).astype(F32), 2)
    counts = jnp.take(row_counts, q_order, axis=0).reshape(1, -1)
    d_order = jnp.bitwise_xor(my_plane, jnp.arange(plane))
    plane_table = jnp.take(lax.dynamic_index_in_dim(table, my_quarter, 0, False), d_order, axis=0)
    d_ids = jnp.concatenate(
        [
            lax.dynamic_index_in_dim(plane_table, my_core, 1, False).reshape(-1),
            lax.dynamic_index_in_dim(plane_table, 1 - my_core, 1, False).reshape(-1),
        ]
    )
    own_ids = lax.dynamic_index_in_dim(q_ids, my_quarter, 0, False)
    positive = (d_ids[:, None] == own_ids[None, :]).astype(F32)

    scores, stats = call(
        functools.partial(score_kernel, scale, rows),
        [((2 * half, cols), F32), ((8, cols), F32)],
        docs,
        q_mine,
        positive,
    )
    stats_all = send_pieces([stats] * quarters, "quarter")
    q_other = swap_cores(q_mine)
    shares = call(
        functools.partial(share_kernel, scale, rows), [piece] * (quarters - 1), scores, stats, docs
    )
    q_got = send_pieces([None] + list(shares), "quarter")

    w_mine, w_send, gains, line_loss = call(
        functools.partial(weight_kernel, batch_rows, rows),
        [((half, cols), BF16), ((half, cols), BF16), ((rows, 8), F32), ((8, 128), F32)],
        scores,
        *stats_all,
        counts,
        total,
        positive,
    )
    w_in = swap_cores(w_send)
    chip_loss = line_loss + swap_cores(line_loss)
    (own_query,) = call(
        functools.partial(own_kernel, scale), [((rows, width), F32)], w_mine, w_send, docs
    )
    spread = plane <= DIRECT
    own_doc, *d_share = call(
        functools.partial(doc_kernel, scale, rows),
        [((rows, width), F32)] + ([piece] * (plane - 1) if spread else [((half, width), BF16)]),
        w_mine,
        w_in,
        q_mine,
        q_other,
    )
    if not spread:
        d_share = [d_share[0][k * rows : (k + 1) * rows] for k in range(1, plane)]
    d_got = send_pieces([d_share[0]] + list(d_share), PLANE)
    plane_loss = tree_sum(send_pieces([chip_loss] * plane, PLANE))
    loss = plane_loss[0, 0] / total[0, 0]
    (doc_grad,) = call(doc_sum_kernel, [piece], own_doc, *d_got[1:])
    (query_grad,) = call(query_sum_kernel, [piece], own_query, gains, *q_got[1:])
    return query_grad, doc_grad, loss


def solution(mesh):
    wide, narrow = mesh.shape["wide"], mesh.shape["narrow"]
    grid = Mesh(mesh.devices.reshape(QUARTERS, wide // QUARTERS, narrow // 2, 2), ALL)

    return jax.shard_map(
        local,
        mesh=grid,
        in_specs=(P(ALL, None), P(ALL, None), P()),
        out_specs=(P(ALL, None), P(ALL, None), P()),
        check_vma=False,
    )
```

```python
import functools
import math

import jax
import jax.numpy as jnp
from jax import lax
from jax.experimental import pallas as pl
from jax.experimental.pallas import tpu as pltpu
from jax.sharding import Mesh, PartitionSpec as P


QUARTERS = 4
ALL = ("quarter", "lane", "chip", "core")
PLANE = ("lane", "chip")
DIRECT = 8
CHUNK = 256
F32, BF16 = jnp.float32, jnp.bfloat16


def send_pieces(pieces, axes):
    count = len(pieces)
    if count <= DIRECT:
        out = [pieces[0]] + [None] * (count - 1)
        for k in range(count - 1, 0, -1):
            out[k] = lax.ppermute(pieces[k], axes, [(i, i ^ k) for i in range(count)])
        return out
    order = jnp.bitwise_xor(lax.axis_index(axes), jnp.arange(count))
    placed = jnp.take(jnp.stack(pieces), order, axis=0)
    moved = jnp.take(lax.all_to_all(placed, axes, 0, 0, tiled=True), order, axis=0)
    return [pieces[0]] + [moved[k] for k in range(1, count)]


def swap_cores(array):
    return lax.ppermute(array, "core", [(0, 1), (1, 0)])


def tree_sum(terms):
    while len(terms) > 1:
        terms = [terms[i] + terms[i + 1] for i in range(0, len(terms), 2)]
    return terms[0]


def contract(a, b, da, db):
    return lax.dot_general(a, b, (((da,), (db,)), ((), ())), preferred_element_type=F32)


def call(kernel, outs, *args, scratch=()):
    vmem = pl.BlockSpec(memory_space=pltpu.VMEM)
    sizes = [a.size * a.dtype.itemsize for a in args]
    sizes += [math.prod(shape) * jnp.dtype(dtype).itemsize for shape, dtype in outs]
    return pl.pallas_call(
        kernel,
        out_shape=[jax.ShapeDtypeStruct(shape, dtype) for shape, dtype in outs],
        in_specs=[vmem] * len(args),
        out_specs=[vmem] * len(outs),
        scratch_shapes=list(scratch),
        compiler_params=pltpu.CompilerParams(vmem_limit_bytes=min(3 * sum(sizes), 40 << 20) + (6 << 20)),
    )(*args)


def spread(line, width):
    lane = lax.broadcasted_iota(jnp.int32, (8, width), 1)
    parts = [jnp.broadcast_to(part.astype(F32)[:, :1], (8, width)) for part in split3(line)]
    value = jnp.where(lane == 0, parts[0], jnp.where(lane == 1, parts[1], jnp.where(lane == 2, parts[2], 0.0)))
    return value.astype(BF16)


def gather3(rows):
    parts = [rows[:, i : i + 1] for i in range(3)]
    return jnp.broadcast_to(join3(*parts), (8, 128))


def each_chunk(total, body):
    if total <= 2 * CHUNK:
        for i in range(total // CHUNK):
            body(i * CHUNK)
    else:

        @pl.loop(0, total // CHUNK)
        def _(i):
            body(pl.multiple_of(i * CHUNK, CHUNK))


def halves(row, core, rows):
    low, high = row[:, :rows], row[:, rows:]
    return jnp.where(core == 0, low, high), jnp.where(core == 0, high, low)


def id_kernel(rows, plane, ids, queries, documents, counts, total, positive, q_own, d_own, found):
    quarters = ids.shape[0] // plane
    my_quarter, my_core = lax.axis_index("quarter"), lax.axis_index("core")
    my_plane = lax.axis_index(PLANE)
    q_own[...] = queries[...]
    d_own[...] = documents[...]
    chips, lanes = ids.shape
    square = ids[...]
    if chips < lanes:
        square = jnp.concatenate([square, jnp.zeros((lanes - chips, lanes), square.dtype)], 0)
    tall = jnp.transpose(square)
    for z in range(quarters):

        def count(chip):
            row = ids[pl.ds(chip, 1), :]
            same = jnp.zeros((lanes, lanes), F32)
            for other in range(z * plane, (z + 1) * plane):
                same += (tall[:, other : other + 1] == row).astype(F32)
            found[pl.ds(chip, 1), :] = jnp.sum(same, 0, keepdims=True)

        if plane <= DIRECT:
            for chip in range(z * plane, (z + 1) * plane):
                count(chip)
        else:
            pl.loop(z * plane, (z + 1) * plane)(count)
    total[...] = jnp.broadcast_to(jnp.sum(jnp.sum(found[...], 0, keepdims=True), 1, keepdims=True), total.shape)
    for k in range(quarters):
        row = found[pl.ds((my_quarter ^ k) * plane + my_plane, 1), :]
        counts[:, k * rows : (k + 1) * rows] = halves(row, my_core, rows)[0]
    own = halves(ids[pl.ds(my_quarter * plane + my_plane, 1), :], my_core, rows)[0]
    for k in range(plane):
        row = ids[pl.ds(my_quarter * plane + (my_plane ^ k), 1), :]
        column = jnp.transpose(jnp.broadcast_to(row, (8, lanes)))[:, :1]
        low, high = (column[:rows] == own).astype(F32), (column[rows:] == own).astype(F32)
        positive[k * rows : (k + 1) * rows, :] = jnp.where(my_core == 0, low, high)
        positive[(plane + k) * rows : (plane + k + 1) * rows, :] = jnp.where(my_core == 0, high, low)


def split3(x):
    high = x.astype(BF16)
    rest = x - high.astype(F32)
    middle = rest.astype(BF16)
    return high, middle, (rest - middle.astype(F32)).astype(BF16)


def join3(high, middle, low):
    return (high.astype(F32) + middle.astype(F32)) + low.astype(F32)


def score_kernel(scale, rows, docs, queries, positive, scores, stats):
    count = docs.shape[0]
    cols = queries.shape[0]
    peak = jnp.full((1, cols), -jnp.inf, F32)
    pos = jnp.zeros((1, rows), F32)
    stats[...] = jnp.zeros(stats.shape, F32)
    stats[0:1, :cols] = peak
    queries_now = queries[...]

    def first(at):
        part = contract(docs[pl.ds(at, CHUNK), :], queries_now, 1, 1) * scale
        scores[pl.ds(at, CHUNK), :] = part
        stats[0:1, :cols] = jnp.maximum(stats[0:1, :cols], jnp.max(part, 0, keepdims=True))
        chosen = jnp.where(positive[pl.ds(at, CHUNK), :] > 0.0, part[:, :rows], 0.0)
        stats[1:2, :rows] += jnp.sum(chosen, 0, keepdims=True)

    each_chunk(count, first)
    peak = stats[0:1, :cols]

    def second(at):
        stats[2:3, :cols] += jnp.sum(jnp.exp(scores[pl.ds(at, CHUNK), :] - peak), 0, keepdims=True)

    each_chunk(count, second)
    stats[0:1, :cols] = peak + jnp.log(stats[2:3, :cols])


def share_kernel(scale, rows, scores, stats, docs, *outs):
    cols = scores.shape[1]
    lse = stats[0:1, :cols]
    total = None
    for at in range(0, scores.shape[0], 2 * CHUNK):
        probs = jnp.exp(scores[at : at + 2 * CHUNK, :] - lse)
        part = contract(jnp.transpose(probs)[rows:].astype(BF16), docs[at : at + 2 * CHUNK, :], 1, 0)
        total = part if total is None else total + part
    total = (total * scale).astype(BF16)
    for k, out in enumerate(outs):
        out[...] = total[k * rows : (k + 1) * rows]


def weight_kernel(batch_rows, rows, scores, s0, s1, s2, s3, counts, total, positive, *outs):
    w_mine, w_send, gains, loss = outs
    tail = w_mine.shape[0]
    cols = scores.shape[1]
    half = scores.shape[0] // 2
    stats = [s[...] for s in (s0, s1, s2, s3)]
    rest = cols // rows
    lses = [
        jnp.concatenate([s[0:1, (k ^ j) * rows : (k ^ j) * rows + rows] for k in range(rest)], 1)
        for j, s in enumerate(stats)
    ]
    top = functools.reduce(jnp.maximum, lses)
    log_denom = top + jnp.log(tree_sum([jnp.exp(a - top) for a in lses]))
    row_counts = counts[...]
    all_pairs = total[...]

    def fill(out, base):
        def body(at):
            src = pl.ds(base + at, CHUNK)
            raw = row_counts * jnp.exp(scores[src, :] - log_denom)
            own = raw[:, : 2 * rows]
            pad = jnp.concatenate([positive[src, :], jnp.zeros((CHUNK, rows), F32)], 1)
            raw = jnp.concatenate([own - pad, raw[:, 2 * rows :]], 1)
            out[pl.ds(at, CHUNK), :] = (batch_rows * raw / all_pairs[:1]).astype(BF16)

        each_chunk(half, body)

    fill(w_send, half)
    fill(w_mine, 0)
    factor = batch_rows * row_counts[:, :rows] / all_pairs[:1, :rows]
    lanes = [factor * jnp.exp(a[:, :rows] - log_denom[:, :rows]) for a in lses]
    tall = jnp.concatenate(lanes + lanes, 0)
    gains[...] = jnp.transpose(jnp.concatenate([tall, tall], 1))[:rows]
    terms = row_counts * log_denom
    line = tree_sum(
        [
            jnp.sum(terms[:, k * rows : (k + 1) * rows] - stats[k][1:2, :rows], 1, keepdims=True)
            for k in range(rest)
        ]
    )
    line = jnp.broadcast_to(line, loss.shape)
    loss[...] = line
    w_send[tail:, :] = spread(line, w_send.shape[1])


def own_kernel(scale, w_mine, w_send, docs, out):
    half = w_mine.shape[0]
    rows = out.shape[0]
    total = None
    for base, ref in ((0, w_mine), (half, w_send)):
        for at in range(0, half, CHUNK):
            w = jnp.transpose(ref[at : at + CHUNK, :128].astype(F32))[:rows].astype(BF16)
            part = contract(w, docs[base + at : base + at + CHUNK, :], 1, 0)
            total = part if total is None else total + part
    out[...] = total * scale


def doc_kernel(scale, rows, w_mine, w_in, q_mine, q_other, loss, own, chip_loss, *outs):
    half = w_mine.shape[0]
    line = loss[...] + gather3(w_in[half:, :])
    chip_loss[...] = line
    note = spread(line, own.shape[1])
    for out in outs:
        out[rows:, :] = note
    for at in range(0, half, CHUNK):
        part = contract(w_mine[at : at + CHUNK, :], q_mine[...], 1, 0)
        part = (part + contract(w_in[at : at + CHUNK, :], q_other[...], 1, 0)) * scale
        for k in range(at // rows, (at + CHUNK) // rows):
            share = part[k * rows - at : (k + 1) * rows - at]
            if k == 0:
                own[...] = share
            else:
                outs[k - 1][:rows, :] = share.astype(BF16)


def query_sum_kernel(own, gains, *refs):
    *got, out = refs
    total = own[...]
    for k, ref in enumerate(got, 1):
        total = total + gains[:, k : k + 1] * ref[...].astype(F32)
    out[...] = total.astype(BF16)


def doc_sum_kernel(own, chip_loss, all_pairs, *refs):
    *got, out, loss = refs
    rows = own.shape[0]
    total = own[...]
    for ref in got:
        total = total + ref[:rows, :].astype(F32)
    out[...] = total.astype(BF16)
    losses = [chip_loss[...]] + [gather3(ref[rows:, :]) for ref in got]
    loss[...] = (tree_sum(losses) / all_pairs[:, :128])[:1]


def local(queries, documents, user_ids):
    rows, width = queries.shape
    quarters = lax.axis_size("quarter")
    plane = lax.axis_size("lane") * lax.axis_size("chip")
    devices = quarters * plane * 2
    batch_rows = float(devices * rows)
    scale = 3.0 / math.sqrt(width)
    cols = quarters * rows
    half = plane * rows
    piece = ((rows, width), BF16)

    d_parts = send_pieces([documents] * plane, PLANE)
    q_parts = send_pieces([queries] * quarters, "quarter")

    counts, total, positive, q_own, d_own = call(
        functools.partial(id_kernel, rows, plane),
        [((1, cols), F32), ((8, cols), F32), ((2 * half, rows), F32), piece, piece],
        user_ids.reshape(quarters * plane, 2 * rows),
        queries,
        documents,
        scratch=[pltpu.VMEM((quarters * plane, 2 * rows), F32)],
    )
    d_parts[0], q_parts[0] = d_own, q_own
    d_mine = jnp.concatenate(d_parts, 0)
    d_other = swap_cores(d_mine)
    q_mine = jnp.concatenate(q_parts, 0)
    docs = jnp.concatenate([d_mine, d_other], 0)

    scores, stats = call(
        functools.partial(score_kernel, scale, rows),
        [((2 * half, cols), F32), ((8, cols), F32)],
        docs,
        q_mine,
        positive,
    )
    stats_all = send_pieces([stats] * quarters, "quarter")
    q_other = swap_cores(q_mine)
    shares = call(functools.partial(share_kernel, scale, rows), [piece] * (quarters - 1), scores, stats, docs)
    q_got = send_pieces([None] + list(shares), "quarter")

    w_mine, w_send, gains, line_loss = call(
        functools.partial(weight_kernel, batch_rows, rows),
        [((half, cols), BF16), ((half + 8, cols), BF16), ((rows, 8), F32), ((8, 128), F32)],
        scores,
        *stats_all,
        counts,
        total,
        positive,
    )
    w_in = swap_cores(w_send)
    (own_query,) = call(functools.partial(own_kernel, scale), [((rows, width), F32)], w_mine, w_send, docs)
    own_doc, chip_loss, *d_share = call(
        functools.partial(doc_kernel, scale, rows),
        [((rows, width), F32), ((8, 128), F32)] + [((rows + 8, width), BF16)] * (plane - 1),
        w_mine,
        w_in,
        q_mine,
        q_other,
        line_loss,
    )
    d_got = send_pieces([d_share[0]] + list(d_share), PLANE)
    doc_grad, loss = call(doc_sum_kernel, [piece, ((1, 128), F32)], own_doc, chip_loss, total, *d_got[1:])
    (query_grad,) = call(query_sum_kernel, [piece], own_query, gains, *q_got[1:])
    return query_grad, doc_grad, loss[0, 0]


def solution(mesh):
    wide, narrow = mesh.shape["wide"], mesh.shape["narrow"]
    grid = Mesh(mesh.devices.reshape(QUARTERS, wide // QUARTERS, narrow // 2, 2), ALL)

    return jax.shard_map(
        local,
        mesh=grid,
        in_specs=(P(ALL, None), P(ALL, None), P()),
        out_specs=(P(ALL, None), P(ALL, None), P()),
        check_vma=False,
    )
```

```python
import functools
import math

import jax
import jax.numpy as jnp
from jax import lax
from jax.experimental import pallas as pl
from jax.experimental.pallas import tpu as pltpu
from jax.sharding import Mesh, PartitionSpec as P


QUARTERS = 4
ALL = ("quarter", "lane", "chip", "core")
PLANE = ("lane", "chip")
DIRECT = 8
CHUNK = 256
LANES = 128
F32, BF16 = jnp.float32, jnp.bfloat16


def send_pieces(pieces, axes):
    count = len(pieces)
    if count <= DIRECT:
        out = [pieces[0]] + [None] * (count - 1)
        for k in range(count - 1, 0, -1):
            out[k] = lax.ppermute(pieces[k], axes, [(i, i ^ k) for i in range(count)])
        return out
    order = jnp.bitwise_xor(lax.axis_index(axes), jnp.arange(count))
    placed = jnp.take(jnp.stack(pieces), order, axis=0)
    moved = jnp.take(lax.all_to_all(placed, axes, 0, 0, tiled=True), order, axis=0)
    return [pieces[0]] + [moved[k] for k in range(1, count)]


def swap_cores(array):
    return lax.ppermute(array, "core", [(0, 1), (1, 0)])


def tree_sum(terms):
    while len(terms) > 1:
        terms = [terms[i] + terms[i + 1] for i in range(0, len(terms), 2)]
    return terms[0]


def contract(a, b, da, db):
    return lax.dot_general(a, b, (((da,), (db,)), ((), ())), preferred_element_type=F32)


def call(kernel, outs, *args, scratch=()):
    vmem = pl.BlockSpec(memory_space=pltpu.VMEM)
    sizes = [a.size * a.dtype.itemsize for a in args]
    sizes += [math.prod(shape) * jnp.dtype(dtype).itemsize for shape, dtype in outs]
    return pl.pallas_call(
        kernel,
        out_shape=[jax.ShapeDtypeStruct(shape, dtype) for shape, dtype in outs],
        in_specs=[vmem] * len(args),
        out_specs=[vmem] * len(outs),
        scratch_shapes=list(scratch),
        compiler_params=pltpu.CompilerParams(vmem_limit_bytes=min(3 * sum(sizes), 40 << 20) + (6 << 20)),
    )(*args)


def spread(line, width):
    lane = lax.broadcasted_iota(jnp.int32, (8, width), 1)
    parts = [jnp.broadcast_to(part.astype(F32)[:, :1], (8, width)) for part in split3(line)]
    value = jnp.where(lane == 0, parts[0], jnp.where(lane == 1, parts[1], jnp.where(lane == 2, parts[2], 0.0)))
    return value.astype(BF16)


def gather3(rows):
    parts = [rows[:, i : i + 1] for i in range(3)]
    return jnp.broadcast_to(join3(*parts), (8, 128))


def each_chunk(total, body):
    if total <= 2 * CHUNK:
        for i in range(total // CHUNK):
            body(i * CHUNK)
    else:

        @pl.loop(0, total // CHUNK)
        def _(i):
            body(pl.multiple_of(i * CHUNK, CHUNK))


def halves(row, core, rows):
    low, high = row[:, :rows], row[:, rows:]
    return jnp.where(core == 0, low, high), jnp.where(core == 0, high, low)


def id_kernel(rows, plane, ids, queries, documents, counts, total, positive, q_own, d_own, found):
    quarters = ids.shape[0] // plane
    my_quarter, my_core = lax.axis_index("quarter"), lax.axis_index("core")
    my_plane = lax.axis_index(PLANE)
    q_own[...] = queries[...]
    d_own[...] = documents[...]
    chips, lanes = ids.shape
    square = ids[...]
    if chips < lanes:
        square = jnp.concatenate([square, jnp.zeros((lanes - chips, lanes), square.dtype)], 0)
    tall = jnp.transpose(square)
    for z in range(quarters):

        def count(chip):
            row = ids[pl.ds(chip, 1), :]
            same = jnp.zeros((lanes, lanes), F32)
            for other in range(z * plane, (z + 1) * plane):
                same += (tall[:, other : other + 1] == row).astype(F32)
            found[pl.ds(chip, 1), :] = jnp.sum(same, 0, keepdims=True)

        if plane <= DIRECT:
            for chip in range(z * plane, (z + 1) * plane):
                count(chip)
        else:
            pl.loop(z * plane, (z + 1) * plane)(count)
    total[...] = jnp.broadcast_to(jnp.sum(jnp.sum(found[...], 0, keepdims=True), 1, keepdims=True), total.shape)
    for k in range(quarters):
        row = found[pl.ds((my_quarter ^ k) * plane + my_plane, 1), :]
        counts[:, k * rows : (k + 1) * rows] = halves(row, my_core, rows)[0]
    own = halves(ids[pl.ds(my_quarter * plane + my_plane, 1), :], my_core, rows)[0]
    for k in range(plane):
        row = ids[pl.ds(my_quarter * plane + (my_plane ^ k), 1), :]
        column = jnp.transpose(jnp.broadcast_to(row, (8, lanes)))[:, :1]
        low, high = (column[:rows] == own).astype(F32), (column[rows:] == own).astype(F32)
        positive[k * rows : (k + 1) * rows, :] = jnp.where(my_core == 0, low, high)
        positive[(plane + k) * rows : (plane + k + 1) * rows, :] = jnp.where(my_core == 0, high, low)


def split3(x):
    high = x.astype(BF16)
    rest = x - high.astype(F32)
    middle = rest.astype(BF16)
    return high, middle, (rest - middle.astype(F32)).astype(BF16)


def join3(high, middle, low):
    return (high.astype(F32) + middle.astype(F32)) + low.astype(F32)


def score_kernel(scale, rows, docs, queries, positive, scores, stats):
    count = docs.shape[0]
    cols = queries.shape[0]
    peak = jnp.full((1, cols), -jnp.inf, F32)
    pos = jnp.zeros((1, rows), F32)
    stats[...] = jnp.zeros(stats.shape, F32)
    stats[0:1, :cols] = peak
    queries_now = queries[...]

    def first(at):
        part = contract(docs[pl.ds(at, CHUNK), :], queries_now, 1, 1) * scale
        scores[pl.ds(at, CHUNK), :] = part
        stats[0:1, :cols] = jnp.maximum(stats[0:1, :cols], jnp.max(part, 0, keepdims=True))
        chosen = jnp.where(positive[pl.ds(at, CHUNK), :] > 0.0, part[:, :rows], 0.0)
        stats[1:2, :rows] += jnp.sum(chosen, 0, keepdims=True)

    each_chunk(count, first)
    peak = stats[0:1, :cols]

    def second(at):
        stats[2:3, :cols] += jnp.sum(jnp.exp(scores[pl.ds(at, CHUNK), :] - peak), 0, keepdims=True)

    each_chunk(count, second)
    stats[0:1, :cols] = peak + jnp.log(stats[2:3, :cols])


def share_kernel(scale, rows, scores, stats, docs, *outs):
    cols = scores.shape[1]
    lse = stats[0:1, :cols]
    total = None
    for at in range(0, scores.shape[0], 2 * CHUNK):
        probs = jnp.exp(scores[at : at + 2 * CHUNK, :] - lse)
        part = contract(jnp.transpose(probs)[rows:].astype(BF16), docs[at : at + 2 * CHUNK, :], 1, 0)
        total = part if total is None else total + part
    total = (total * scale).astype(BF16)
    for k, out in enumerate(outs):
        out[...] = total[k * rows : (k + 1) * rows]


def weight_kernel(batch_rows, rows, scores, s0, s1, s2, s3, counts, total, positive, *outs):
    w_mine, w_send, gains, loss = outs
    tail = w_mine.shape[0]
    cols = scores.shape[1]
    half = scores.shape[0] // 2
    stats = [s[...] for s in (s0, s1, s2, s3)]
    rest = cols // rows
    lses = [
        jnp.concatenate([s[0:1, (k ^ j) * rows : (k ^ j) * rows + rows] for k in range(rest)], 1)
        for j, s in enumerate(stats)
    ]
    top = functools.reduce(jnp.maximum, lses)
    log_denom = top + jnp.log(tree_sum([jnp.exp(a - top) for a in lses]))
    row_counts = counts[...]
    all_pairs = total[...]

    def fill(out, base):
        def body(at):
            src = pl.ds(base + at, CHUNK)
            raw = row_counts * jnp.exp(scores[src, :] - log_denom)
            own = raw[:, : 2 * rows]
            pad = jnp.concatenate([positive[src, :], jnp.zeros((CHUNK, rows), F32)], 1)
            raw = jnp.concatenate([own - pad, raw[:, 2 * rows :]], 1)
            out[pl.ds(at, CHUNK), :] = (batch_rows * raw / all_pairs[:1]).astype(BF16)

        each_chunk(half, body)

    fill(w_send, half)
    fill(w_mine, 0)
    factor = batch_rows * row_counts[:, :rows] / all_pairs[:1, :rows]
    lanes = [factor * jnp.exp(a[:, :rows] - log_denom[:, :rows]) for a in lses]
    tall = jnp.concatenate(lanes + lanes, 0)
    gains[...] = jnp.transpose(jnp.concatenate([tall, tall], 1))[:rows]
    terms = row_counts * log_denom
    line = tree_sum(
        [
            jnp.sum(terms[:, k * rows : (k + 1) * rows] - stats[k][1:2, :rows], 1, keepdims=True)
            for k in range(rest)
        ]
    )
    line = jnp.broadcast_to(line, loss.shape)
    loss[...] = line
    w_send[tail:, :] = spread(line, w_send.shape[1])


def own_kernel(scale, w_mine, w_send, docs, out):
    half = w_mine.shape[0]
    rows = out.shape[0]
    total = None
    for base, ref in ((0, w_mine), (half, w_send)):
        for at in range(0, half, CHUNK):
            w = jnp.transpose(ref[at : at + CHUNK, :128].astype(F32))[:rows].astype(BF16)
            part = contract(w, docs[base + at : base + at + CHUNK, :], 1, 0)
            total = part if total is None else total + part
    out[...] = total * scale


def doc_kernel(scale, rows, w_mine, w_in, q_mine, q_other, loss, own, chip_loss, *outs):
    half = w_mine.shape[0]
    line = loss[...] + gather3(w_in[half:, :])
    chip_loss[...] = line
    tiles = own.shape[1] // LANES
    note = spread(line, LANES)
    for out in outs:
        out[tiles * rows :, :] = note
    for at in range(0, half, CHUNK):
        part = contract(w_mine[at : at + CHUNK, :], q_mine[...], 1, 0)
        part = (part + contract(w_in[at : at + CHUNK, :], q_other[...], 1, 0)) * scale
        for k in range(at // rows, (at + CHUNK) // rows):
            share = part[k * rows - at : (k + 1) * rows - at]
            if k == 0:
                own[...] = share
            else:
                for t in range(tiles):
                    outs[k - 1][t * rows : (t + 1) * rows, :] = share[:, t * LANES : (t + 1) * LANES].astype(BF16)


def query_sum_kernel(own, gains, *refs):
    *got, out = refs
    total = own[...]
    for k, ref in enumerate(got, 1):
        total = total + gains[:, k : k + 1] * ref[...].astype(F32)
    out[...] = total.astype(BF16)


def doc_sum_kernel(own, chip_loss, all_pairs, *refs):
    *got, out, loss = refs
    rows = own.shape[0]
    tiles = own.shape[1] // LANES
    for t in range(tiles):
        total = own[:, t * LANES : (t + 1) * LANES]
        for ref in got:
            total = total + ref[t * rows : (t + 1) * rows, :].astype(F32)
        out[:, t * LANES : (t + 1) * LANES] = total.astype(BF16)
    losses = [chip_loss[...]] + [gather3(ref[tiles * rows :, :]) for ref in got]
    loss[...] = (tree_sum(losses) / all_pairs[:, :128])[:1]


def local(queries, documents, user_ids):
    rows, width = queries.shape
    quarters = lax.axis_size("quarter")
    plane = lax.axis_size("lane") * lax.axis_size("chip")
    devices = quarters * plane * 2
    batch_rows = float(devices * rows)
    scale = 3.0 / math.sqrt(width)
    cols = quarters * rows
    half = plane * rows
    piece = ((rows, width), BF16)

    d_parts = send_pieces([documents] * plane, PLANE)
    q_parts = send_pieces([queries] * quarters, "quarter")

    counts, total, positive, q_own, d_own = call(
        functools.partial(id_kernel, rows, plane),
        [((1, cols), F32), ((8, cols), F32), ((2 * half, rows), F32), piece, piece],
        user_ids.reshape(quarters * plane, 2 * rows),
        queries,
        documents,
        scratch=[pltpu.VMEM((quarters * plane, 2 * rows), F32)],
    )
    d_parts[0], q_parts[0] = d_own, q_own
    d_mine = jnp.concatenate(d_parts, 0)
    d_other = swap_cores(d_mine)
    q_mine = jnp.concatenate(q_parts, 0)
    docs = jnp.concatenate([d_mine, d_other], 0)

    scores, stats = call(
        functools.partial(score_kernel, scale, rows),
        [((2 * half, cols), F32), ((8, cols), F32)],
        docs,
        q_mine,
        positive,
    )
    stats_all = send_pieces([stats] * quarters, "quarter")
    q_other = swap_cores(q_mine)
    shares = call(functools.partial(share_kernel, scale, rows), [piece] * (quarters - 1), scores, stats, docs)
    q_got = send_pieces([None] + list(shares), "quarter")

    w_mine, w_send, gains, line_loss = call(
        functools.partial(weight_kernel, batch_rows, rows),
        [((half, cols), BF16), ((half + 8, cols), BF16), ((rows, 8), F32), ((8, 128), F32)],
        scores,
        *stats_all,
        counts,
        total,
        positive,
    )
    w_in = swap_cores(w_send)
    (own_query,) = call(functools.partial(own_kernel, scale), [((rows, width), F32)], w_mine, w_send, docs)
    own_doc, chip_loss, *d_share = call(
        functools.partial(doc_kernel, scale, rows),
        [((rows, width), F32), ((8, 128), F32)] + [((rows * width // LANES + 8, LANES), BF16)] * (plane - 1),
        w_mine,
        w_in,
        q_mine,
        q_other,
        line_loss,
    )
    d_got = send_pieces([d_share[0]] + list(d_share), PLANE)
    doc_grad, loss = call(doc_sum_kernel, [piece, ((1, 128), F32)], own_doc, chip_loss, total, *d_got[1:])
    (query_grad,) = call(query_sum_kernel, [piece], own_query, gains, *q_got[1:])
    return query_grad, doc_grad, loss[0, 0]


def solution(mesh):
    wide, narrow = mesh.shape["wide"], mesh.shape["narrow"]
    grid = Mesh(mesh.devices.reshape(QUARTERS, wide // QUARTERS, narrow // 2, 2), ALL)

    return jax.shard_map(
        local,
        mesh=grid,
        in_specs=(P(ALL, None), P(ALL, None), P()),
        out_specs=(P(ALL, None), P(ALL, None), P()),
        check_vma=False,
    )
```

```python
import functools
import math

import jax
import jax.numpy as jnp
from jax import lax
from jax.experimental import pallas as pl
from jax.experimental.pallas import tpu as pltpu
from jax.sharding import Mesh, PartitionSpec as P


QUARTERS = 4
ALL = ("quarter", "lane", "chip", "core")
PLANE = ("lane", "chip")
DIRECT = 8
CHUNK = 256
LANES = 128
F32, BF16 = jnp.float32, jnp.bfloat16


def send_pieces(pieces, axes):
    count = len(pieces)
    if count <= DIRECT:
        out = [pieces[0]] + [None] * (count - 1)
        for k in range(count - 1, 0, -1):
            out[k] = lax.ppermute(pieces[k], axes, [(i, i ^ k) for i in range(count)])
        return out
    order = jnp.bitwise_xor(lax.axis_index(axes), jnp.arange(count))
    placed = jnp.take(jnp.stack(pieces), order, axis=0)
    moved = jnp.take(lax.all_to_all(placed, axes, 0, 0, tiled=True), order, axis=0)
    return [pieces[0]] + [moved[k] for k in range(1, count)]


def swap_cores(array):
    return lax.ppermute(array, "core", [(0, 1), (1, 0)])


def tree_sum(terms):
    while len(terms) > 1:
        terms = [terms[i] + terms[i + 1] for i in range(0, len(terms), 2)]
    return terms[0]


def contract(a, b, da, db):
    return lax.dot_general(a, b, (((da,), (db,)), ((), ())), preferred_element_type=F32)


def piece_order(plane):
    return [0] + list(range(plane - 1, 0, -1))


def call(kernel, outs, *args, scratch=(), in_hbm=False):
    vmem = pl.BlockSpec(memory_space=pltpu.VMEM)
    sizes = [a.size * a.dtype.itemsize for a in args]
    sizes += [math.prod(shape) * jnp.dtype(dtype).itemsize for shape, dtype in outs]
    return pl.pallas_call(
        kernel,
        out_shape=[jax.ShapeDtypeStruct(shape, dtype) for shape, dtype in outs],
        in_specs=[pl.BlockSpec(memory_space=pl.ANY) if in_hbm else vmem] * len(args),
        out_specs=[vmem] * len(outs),
        scratch_shapes=list(scratch),
        compiler_params=pltpu.CompilerParams(vmem_limit_bytes=min(3 * sum(sizes), 40 << 20) + (6 << 20)),
    )(*args)


def spread(line, width):
    lane = lax.broadcasted_iota(jnp.int32, (8, width), 1)
    parts = [jnp.broadcast_to(part.astype(F32)[:, :1], (8, width)) for part in split3(line)]
    value = jnp.where(lane == 0, parts[0], jnp.where(lane == 1, parts[1], jnp.where(lane == 2, parts[2], 0.0)))
    return value.astype(BF16)


def gather3(rows):
    parts = [rows[:, i : i + 1] for i in range(3)]
    return jnp.broadcast_to(join3(*parts), (8, 128))


def each_chunk(total, body):
    if total <= 2 * CHUNK:
        for i in range(total // CHUNK):
            body(i * CHUNK)
    else:

        @pl.loop(0, total // CHUNK)
        def _(i):
            body(pl.multiple_of(i * CHUNK, CHUNK))


def halves(row, core, rows):
    low, high = row[:, :rows], row[:, rows:]
    return jnp.where(core == 0, low, high), jnp.where(core == 0, high, low)


def id_kernel(rows, plane, ids_in, queries, documents, counts, total, positive, q_own, d_own, found, ids, sems):
    quarters = ids.shape[0] // plane
    my_quarter, my_core = lax.axis_index("quarter"), lax.axis_index("core")
    my_plane = lax.axis_index(PLANE)
    copies = [
        pltpu.make_async_copy(src, dst, sems.at[i])
        for i, (src, dst) in enumerate(((ids_in, ids), (documents, d_own), (queries, q_own)))
    ]
    for copy in copies:
        copy.start()
    copies[0].wait()
    chips, lanes = ids.shape
    square = ids[...]
    if chips < lanes:
        square = jnp.concatenate([square, jnp.zeros((lanes - chips, lanes), square.dtype)], 0)
    tall = jnp.transpose(square)
    for z in range(quarters):

        def count(chip):
            row = ids[pl.ds(chip, 1), :]
            same = jnp.zeros((lanes, lanes), F32)
            for other in range(z * plane, (z + 1) * plane):
                same += (tall[:, other : other + 1] == row).astype(F32)
            found[pl.ds(chip, 1), :] = jnp.sum(same, 0, keepdims=True)

        if plane <= DIRECT:
            for chip in range(z * plane, (z + 1) * plane):
                count(chip)
        else:
            pl.loop(z * plane, (z + 1) * plane)(count)
    total[...] = jnp.broadcast_to(jnp.sum(jnp.sum(found[...], 0, keepdims=True), 1, keepdims=True), total.shape)
    for k in range(quarters):
        row = found[pl.ds((my_quarter ^ k) * plane + my_plane, 1), :]
        counts[:, k * rows : (k + 1) * rows] = halves(row, my_core, rows)[0]
    own = halves(ids[pl.ds(my_quarter * plane + my_plane, 1), :], my_core, rows)[0]
    for k, piece in enumerate(piece_order(plane)):
        row = ids[pl.ds(my_quarter * plane + (my_plane ^ piece), 1), :]
        column = jnp.transpose(jnp.broadcast_to(row, (8, lanes)))[:, :1]
        low, high = (column[:rows] == own).astype(F32), (column[rows:] == own).astype(F32)
        positive[k * rows : (k + 1) * rows, :] = jnp.where(my_core == 0, low, high)
        positive[(plane + k) * rows : (plane + k + 1) * rows, :] = jnp.where(my_core == 0, high, low)
    for copy in copies[1:]:
        copy.wait()


def split3(x):
    high = x.astype(BF16)
    rest = x - high.astype(F32)
    middle = rest.astype(BF16)
    return high, middle, (rest - middle.astype(F32)).astype(BF16)


def join3(high, middle, low):
    return (high.astype(F32) + middle.astype(F32)) + low.astype(F32)


def score_kernel(scale, rows, docs, queries, positive, scores, stats):
    count = docs.shape[0]
    cols = queries.shape[0]
    peak = jnp.full((1, cols), -jnp.inf, F32)
    pos = jnp.zeros((1, rows), F32)
    stats[...] = jnp.zeros(stats.shape, F32)
    stats[0:1, :cols] = peak
    queries_now = queries[...]

    def first(at):
        part = contract(docs[pl.ds(at, CHUNK), :], queries_now, 1, 1) * scale
        scores[pl.ds(at, CHUNK), :] = part
        stats[0:1, :cols] = jnp.maximum(stats[0:1, :cols], jnp.max(part, 0, keepdims=True))
        chosen = jnp.where(positive[pl.ds(at, CHUNK), :] > 0.0, part[:, :rows], 0.0)
        stats[1:2, :rows] += jnp.sum(chosen, 0, keepdims=True)

    each_chunk(count, first)
    peak = stats[0:1, :cols]

    def second(at):
        stats[2:3, :cols] += jnp.sum(jnp.exp(scores[pl.ds(at, CHUNK), :] - peak), 0, keepdims=True)

    each_chunk(count, second)
    stats[0:1, :cols] = peak + jnp.log(stats[2:3, :cols])


def share_kernel(scale, rows, scores, stats, docs, *outs):
    cols = scores.shape[1]
    lse = stats[0:1, :cols]
    total = None
    for at in range(0, scores.shape[0], 2 * CHUNK):
        probs = jnp.exp(scores[at : at + 2 * CHUNK, :] - lse)
        part = contract(jnp.transpose(probs)[rows:].astype(BF16), docs[at : at + 2 * CHUNK, :], 1, 0)
        total = part if total is None else total + part
    total = (total * scale).astype(BF16)
    for k, out in enumerate(outs):
        out[...] = total[k * rows : (k + 1) * rows]


def weight_kernel(batch_rows, rows, scores, s0, s1, s2, s3, counts, total, positive, *outs):
    w_mine, w_send, gains, loss = outs
    tail = w_mine.shape[0]
    cols = scores.shape[1]
    half = scores.shape[0] // 2
    stats = [s[...] for s in (s0, s1, s2, s3)]
    rest = cols // rows
    lses = [
        jnp.concatenate([s[0:1, (k ^ j) * rows : (k ^ j) * rows + rows] for k in range(rest)], 1)
        for j, s in enumerate(stats)
    ]
    top = functools.reduce(jnp.maximum, lses)
    log_denom = top + jnp.log(tree_sum([jnp.exp(a - top) for a in lses]))
    row_counts = counts[...]
    all_pairs = total[...]

    def fill(out, base):
        def body(at):
            src = pl.ds(base + at, CHUNK)
            raw = row_counts * jnp.exp(scores[src, :] - log_denom)
            own = raw[:, : 2 * rows]
            pad = jnp.concatenate([positive[src, :], jnp.zeros((CHUNK, rows), F32)], 1)
            raw = jnp.concatenate([own - pad, raw[:, 2 * rows :]], 1)
            out[pl.ds(at, CHUNK), :] = (batch_rows * raw / all_pairs[:1]).astype(BF16)

        each_chunk(half, body)

    fill(w_send, half)
    fill(w_mine, 0)
    factor = batch_rows * row_counts[:, :rows] / all_pairs[:1, :rows]
    lanes = [factor * jnp.exp(a[:, :rows] - log_denom[:, :rows]) for a in lses]
    tall = jnp.concatenate(lanes + lanes, 0)
    gains[...] = jnp.transpose(jnp.concatenate([tall, tall], 1))[:rows]
    terms = row_counts * log_denom
    line = tree_sum(
        [
            jnp.sum(terms[:, k * rows : (k + 1) * rows] - stats[k][1:2, :rows], 1, keepdims=True)
            for k in range(rest)
        ]
    )
    line = jnp.broadcast_to(line, loss.shape)
    loss[...] = line
    w_send[tail:, :] = spread(line, w_send.shape[1])


def own_kernel(scale, w_mine, w_send, docs, out):
    half = w_mine.shape[0]
    rows = out.shape[0]
    total = None
    for base, ref in ((0, w_mine), (half, w_send)):
        for at in range(0, half, CHUNK):
            w = jnp.transpose(ref[at : at + CHUNK, :128].astype(F32))[:rows].astype(BF16)
            part = contract(w, docs[base + at : base + at + CHUNK, :], 1, 0)
            total = part if total is None else total + part
    out[...] = total * scale


def doc_kernel(scale, rows, w_mine, w_in, q_mine, q_other, loss, own, chip_loss, *outs):
    half = w_mine.shape[0]
    line = loss[...] + gather3(w_in[half:, :])
    chip_loss[...] = line
    tiles = own.shape[1] // LANES
    note = spread(line, LANES)
    order = piece_order(half // rows)
    for out in outs:
        out[tiles * rows :, :] = note
    for at in range(0, half, CHUNK):
        part = contract(w_mine[at : at + CHUNK, :], q_mine[...], 1, 0)
        part = (part + contract(w_in[at : at + CHUNK, :], q_other[...], 1, 0)) * scale
        for j in range(at // rows, (at + CHUNK) // rows):
            share = part[j * rows - at : (j + 1) * rows - at]
            k = order[j]
            if k == 0:
                own[...] = share
            else:
                for t in range(tiles):
                    outs[k - 1][t * rows : (t + 1) * rows, :] = share[:, t * LANES : (t + 1) * LANES].astype(BF16)


def sum_kernel(peers, own_query, gains, own, chip_loss, all_pairs, *refs):
    *got, query_out, doc_out, loss = refs
    q_got, d_got = got[:peers], got[peers:]
    rows = own.shape[0]
    tiles = own.shape[1] // LANES
    gain = [gains[:, k : k + 1] for k in range(peers + 1)]
    for t in range(tiles):
        lanes = slice(t * LANES, (t + 1) * LANES)
        total = own_query[:, lanes]
        for k, ref in enumerate(q_got, 1):
            total = total + gain[k] * ref[:, lanes].astype(F32)
        query_out[:, lanes] = total.astype(BF16)
        total = own[:, lanes]
        for ref in d_got:
            total = total + ref[t * rows : (t + 1) * rows, :].astype(F32)
        doc_out[:, lanes] = total.astype(BF16)
    losses = [chip_loss[...]] + [gather3(ref[tiles * rows :, :]) for ref in d_got]
    loss[...] = (tree_sum(losses) / all_pairs[:, :128])[:1]


def local(queries, documents, user_ids):
    rows, width = queries.shape
    quarters = lax.axis_size("quarter")
    plane = lax.axis_size("lane") * lax.axis_size("chip")
    devices = quarters * plane * 2
    batch_rows = float(devices * rows)
    scale = 3.0 / math.sqrt(width)
    cols = quarters * rows
    half = plane * rows
    piece = ((rows, width), BF16)

    d_parts = send_pieces([documents] * plane, PLANE)
    q_parts = send_pieces([queries] * quarters, "quarter")

    counts, total, positive, q_own, d_own = call(
        functools.partial(id_kernel, rows, plane),
        [((1, cols), F32), ((8, cols), F32), ((2 * half, rows), F32), piece, piece],
        user_ids.reshape(quarters * plane, 2 * rows),
        queries,
        documents,
        scratch=[
            pltpu.VMEM((quarters * plane, 2 * rows), F32),
            pltpu.VMEM((quarters * plane, 2 * rows), user_ids.dtype),
            pltpu.SemaphoreType.DMA((3,)),
        ],
        in_hbm=True,
    )
    d_parts[0], q_parts[0] = d_own, q_own
    d_parts = [d_parts[k] for k in piece_order(plane)]
    d_first = jnp.concatenate(d_parts[:-1], 0)
    first_other = swap_cores(d_first)
    last_other = swap_cores(d_parts[-1])
    q_mine = jnp.concatenate(q_parts, 0)
    docs = jnp.concatenate([d_first, d_parts[-1], first_other, last_other], 0)

    scores, stats = call(
        functools.partial(score_kernel, scale, rows),
        [((2 * half, cols), F32), ((8, cols), F32)],
        docs,
        q_mine,
        positive,
    )
    stats_all = send_pieces([stats] * quarters, "quarter")
    q_other = swap_cores(q_mine)
    shares = call(functools.partial(share_kernel, scale, rows), [piece] * (quarters - 1), scores, stats, docs)
    q_got = send_pieces([None] + list(shares), "quarter")

    w_mine, w_send, gains, line_loss = call(
        functools.partial(weight_kernel, batch_rows, rows),
        [((half, cols), BF16), ((half + 8, cols), BF16), ((rows, 8), F32), ((8, 128), F32)],
        scores,
        *stats_all,
        counts,
        total,
        positive,
    )
    w_in = swap_cores(w_send)
    (own_query,) = call(functools.partial(own_kernel, scale), [((rows, width), F32)], w_mine, w_send, docs)
    own_doc, chip_loss, *d_share = call(
        functools.partial(doc_kernel, scale, rows),
        [((rows, width), F32), ((8, 128), F32)] + [((rows * width // LANES + 8, LANES), BF16)] * (plane - 1),
        w_mine,
        w_in,
        q_mine,
        q_other,
        line_loss,
    )
    d_got = send_pieces([d_share[0]] + list(d_share), PLANE)
    query_grad, doc_grad, loss = call(
        functools.partial(sum_kernel, quarters - 1),
        [piece, piece, ((1, 128), F32)],
        own_query,
        gains,
        own_doc,
        chip_loss,
        total,
        *q_got[1:],
        *d_got[1:],
    )
    return query_grad, doc_grad, loss[0, 0]


def solution(mesh):
    wide, narrow = mesh.shape["wide"], mesh.shape["narrow"]
    grid = Mesh(mesh.devices.reshape(QUARTERS, wide // QUARTERS, narrow // 2, 2), ALL)

    return jax.shard_map(
        local,
        mesh=grid,
        in_specs=(P(ALL, None), P(ALL, None), P()),
        out_specs=(P(ALL, None), P(ALL, None), P()),
        check_vma=False,
    )
```

```python
import functools
import math

import jax
import jax.numpy as jnp
from jax import lax
from jax.experimental import pallas as pl
from jax.experimental.pallas import tpu as pltpu
from jax.sharding import Mesh, PartitionSpec as P


QUARTERS = 4
ALL = ("quarter", "lane", "chip", "core")
PLANE = ("lane", "chip")
DIRECT = 8
CHUNK = 256
LANES = 128
F32, BF16 = jnp.float32, jnp.bfloat16


def send_pieces(pieces, axes):
    count = len(pieces)
    if count <= DIRECT:
        out = [pieces[0]] + [None] * (count - 1)
        for k in range(count - 1, 0, -1):
            out[k] = lax.ppermute(pieces[k], axes, [(i, i ^ k) for i in range(count)])
        return out
    order = jnp.bitwise_xor(lax.axis_index(axes), jnp.arange(count))
    placed = jnp.take(jnp.stack(pieces), order, axis=0)
    moved = jnp.take(lax.all_to_all(placed, axes, 0, 0, tiled=True), order, axis=0)
    return [pieces[0]] + [moved[k] for k in range(1, count)]


def swap_cores(array):
    return lax.ppermute(array, "core", [(0, 1), (1, 0)])


def tree_sum(terms):
    while len(terms) > 1:
        terms = [terms[i] + terms[i + 1] for i in range(0, len(terms), 2)]
    return terms[0]


def contract(a, b, da, db):
    return lax.dot_general(a, b, (((da,), (db,)), ((), ())), preferred_element_type=F32)


def piece_order(plane):
    return [0] + list(range(plane - 1, 0, -1))


def call(kernel, outs, *args, scratch=(), in_hbm=False):
    vmem = pl.BlockSpec(memory_space=pltpu.VMEM)
    sizes = [a.size * a.dtype.itemsize for a in args]
    sizes += [math.prod(shape) * jnp.dtype(dtype).itemsize for shape, dtype in outs]
    return pl.pallas_call(
        kernel,
        out_shape=[jax.ShapeDtypeStruct(shape, dtype) for shape, dtype in outs],
        in_specs=[pl.BlockSpec(memory_space=pl.ANY) if in_hbm else vmem] * len(args),
        out_specs=[vmem] * len(outs),
        scratch_shapes=list(scratch),
        compiler_params=pltpu.CompilerParams(vmem_limit_bytes=min(3 * sum(sizes), 40 << 20) + (6 << 20)),
    )(*args)


def spread(line, width):
    lane = lax.broadcasted_iota(jnp.int32, (8, width), 1)
    parts = [jnp.broadcast_to(part.astype(F32)[:, :1], (8, width)) for part in split3(line)]
    value = jnp.where(lane == 0, parts[0], jnp.where(lane == 1, parts[1], jnp.where(lane == 2, parts[2], 0.0)))
    return value.astype(BF16)


def gather3(rows):
    parts = [rows[:, i : i + 1] for i in range(3)]
    return jnp.broadcast_to(join3(*parts), (8, 128))


def each_chunk(total, body):
    if total <= 2 * CHUNK:
        for i in range(total // CHUNK):
            body(i * CHUNK)
    else:

        @pl.loop(0, total // CHUNK)
        def _(i):
            body(pl.multiple_of(i * CHUNK, CHUNK))


def halves(row, core, rows):
    low, high = row[:, :rows], row[:, rows:]
    return jnp.where(core == 0, low, high), jnp.where(core == 0, high, low)


def id_kernel(rows, plane, ids_in, queries, documents, counts, total, positive, q_own, d_own, found, ids, sems):
    quarters = ids.shape[0] // plane
    my_quarter, my_core = lax.axis_index("quarter"), lax.axis_index("core")
    my_plane = lax.axis_index(PLANE)
    copies = [
        pltpu.make_async_copy(src, dst, sems.at[i])
        for i, (src, dst) in enumerate(((ids_in, ids), (documents, d_own), (queries, q_own)))
    ]
    for copy in copies:
        copy.start()
    copies[0].wait()
    chips, lanes = ids.shape
    square = ids[...]
    if chips < lanes:
        square = jnp.concatenate([square, jnp.zeros((lanes - chips, lanes), square.dtype)], 0)
    tall = jnp.transpose(square)
    for z in range(quarters):

        def count(chip):
            row = ids[pl.ds(chip, 1), :]
            same = jnp.zeros((lanes, lanes), F32)
            for other in range(z * plane, (z + 1) * plane):
                same += (tall[:, other : other + 1] == row).astype(F32)
            found[pl.ds(chip, 1), :] = jnp.sum(same, 0, keepdims=True)

        if plane <= DIRECT:
            for chip in range(z * plane, (z + 1) * plane):
                count(chip)
        else:
            pl.loop(z * plane, (z + 1) * plane)(count)
    total[...] = jnp.broadcast_to(jnp.sum(jnp.sum(found[...], 0, keepdims=True), 1, keepdims=True), total.shape)
    for k in range(quarters):
        row = found[pl.ds((my_quarter ^ k) * plane + my_plane, 1), :]
        counts[:, k * rows : (k + 1) * rows] = halves(row, my_core, rows)[0]
    own = halves(ids[pl.ds(my_quarter * plane + my_plane, 1), :], my_core, rows)[0]
    for k, piece in enumerate(piece_order(plane)):
        row = ids[pl.ds(my_quarter * plane + (my_plane ^ piece), 1), :]
        column = jnp.transpose(jnp.broadcast_to(row, (8, lanes)))[:, :1]
        low, high = (column[:rows] == own).astype(F32), (column[rows:] == own).astype(F32)
        positive[k * rows : (k + 1) * rows, :] = jnp.where(my_core == 0, low, high)
        positive[(plane + k) * rows : (plane + k + 1) * rows, :] = jnp.where(my_core == 0, high, low)
    for copy in copies[1:]:
        copy.wait()


def split3(x):
    high = x.astype(BF16)
    rest = x - high.astype(F32)
    middle = rest.astype(BF16)
    return high, middle, (rest - middle.astype(F32)).astype(BF16)


def join3(high, middle, low):
    return (high.astype(F32) + middle.astype(F32)) + low.astype(F32)


def score_kernel(scale, rows, docs, queries, positive, scores, stats):
    count = docs.shape[0]
    cols = queries.shape[0]
    peak = jnp.full((1, cols), -jnp.inf, F32)
    pos = jnp.zeros((1, rows), F32)
    stats[...] = jnp.zeros(stats.shape, F32)
    stats[0:1, :cols] = peak
    queries_now = queries[...]

    def first(at):
        part = contract(docs[pl.ds(at, CHUNK), :], queries_now, 1, 1) * scale
        scores[pl.ds(at, CHUNK), :] = part
        stats[0:1, :cols] = jnp.maximum(stats[0:1, :cols], jnp.max(part, 0, keepdims=True))
        chosen = jnp.where(positive[pl.ds(at, CHUNK), :] > 0.0, part[:, :rows], 0.0)
        stats[1:2, :rows] += jnp.sum(chosen, 0, keepdims=True)

    each_chunk(count, first)
    peak = stats[0:1, :cols]

    def second(at):
        stats[2:3, :cols] += jnp.sum(jnp.exp(scores[pl.ds(at, CHUNK), :] - peak), 0, keepdims=True)

    each_chunk(count, second)
    stats[0:1, :cols] = peak + jnp.log(stats[2:3, :cols])


def share_kernel(scale, rows, scores, stats, docs, *outs):
    cols = scores.shape[1]
    lse = stats[0:1, :cols]
    total = None
    for at in range(0, scores.shape[0], 2 * CHUNK):
        probs = jnp.exp(scores[at : at + 2 * CHUNK, :] - lse)
        part = contract(jnp.transpose(probs)[rows:].astype(BF16), docs[at : at + 2 * CHUNK, :], 1, 0)
        total = part if total is None else total + part
    total = (total * scale).astype(BF16)
    for k, out in enumerate(outs):
        out[...] = total[k * rows : (k + 1) * rows]


def weight_kernel(batch_rows, rows, scores, s0, s1, s2, s3, counts, total, positive, *outs):
    w_mine, w_send, gains, loss = outs
    tail = w_mine.shape[0]
    cols = scores.shape[1]
    half = scores.shape[0] // 2
    stats = [s[...] for s in (s0, s1, s2, s3)]
    rest = cols // rows
    lses = [
        jnp.concatenate([s[0:1, (k ^ j) * rows : (k ^ j) * rows + rows] for k in range(rest)], 1)
        for j, s in enumerate(stats)
    ]
    top = functools.reduce(jnp.maximum, lses)
    log_denom = top + jnp.log(tree_sum([jnp.exp(a - top) for a in lses]))
    row_counts = counts[...]
    per_pair = batch_rows / total[:1, :]

    def fill(out, base):
        def body(at):
            src = pl.ds(base + at, CHUNK)
            raw = row_counts * jnp.exp(scores[src, :] - log_denom)
            own = raw[:, : 2 * rows]
            pad = jnp.concatenate([positive[src, :], jnp.zeros((CHUNK, rows), F32)], 1)
            raw = jnp.concatenate([own - pad, raw[:, 2 * rows :]], 1)
            out[pl.ds(at, CHUNK), :] = (raw * per_pair).astype(BF16)

        each_chunk(half, body)

    fill(w_send, half)
    fill(w_mine, 0)
    factor = row_counts[:, :rows] * per_pair[:, :rows]
    lanes = [factor * jnp.exp(a[:, :rows] - log_denom[:, :rows]) for a in lses]
    tall = jnp.concatenate(lanes + lanes, 0)
    gains[...] = jnp.transpose(jnp.concatenate([tall, tall], 1))[:rows]
    terms = row_counts * log_denom
    line = tree_sum(
        [
            jnp.sum(terms[:, k * rows : (k + 1) * rows] - stats[k][1:2, :rows], 1, keepdims=True)
            for k in range(rest)
        ]
    )
    line = jnp.broadcast_to(line, loss.shape)
    loss[...] = line
    w_send[tail:, :] = spread(line, w_send.shape[1])


def own_kernel(scale, w_mine, w_send, docs, out):
    half = w_mine.shape[0]
    rows = out.shape[0]
    total = None
    for base, ref in ((0, w_mine), (half, w_send)):
        for at in range(0, half, CHUNK):
            w = jnp.transpose(ref[at : at + CHUNK, :128].astype(F32))[:rows].astype(BF16)
            part = contract(w, docs[base + at : base + at + CHUNK, :], 1, 0)
            total = part if total is None else total + part
    out[...] = total * scale


def doc_kernel(scale, rows, w_mine, w_in, q_mine, q_other, loss, own, chip_loss, *outs):
    half = w_mine.shape[0]
    line = loss[...] + gather3(w_in[half:, :])
    chip_loss[...] = line
    tiles = own.shape[1] // LANES
    note = spread(line, LANES)
    order = piece_order(half // rows)
    for out in outs:
        out[tiles * rows :, :] = note
    for at in range(0, half, CHUNK):
        part = contract(w_mine[at : at + CHUNK, :], q_mine[...], 1, 0)
        part = (part + contract(w_in[at : at + CHUNK, :], q_other[...], 1, 0)) * scale
        for j in range(at // rows, (at + CHUNK) // rows):
            share = part[j * rows - at : (j + 1) * rows - at]
            k = order[j]
            if k == 0:
                own[...] = share
            else:
                for t in range(tiles):
                    outs[k - 1][t * rows : (t + 1) * rows, :] = share[:, t * LANES : (t + 1) * LANES].astype(BF16)


def sum_kernel(peers, own_query, gains, own, chip_loss, all_pairs, *refs):
    *got, query_out, doc_out, loss = refs
    q_got, d_got = got[:peers], got[peers:]
    rows = own.shape[0]
    tiles = own.shape[1] // LANES
    gain = [gains[:, k : k + 1] for k in range(peers + 1)]
    for t in range(tiles):
        lanes = slice(t * LANES, (t + 1) * LANES)
        total = own_query[:, lanes]
        for k, ref in enumerate(q_got, 1):
            total = total + gain[k] * ref[:, lanes].astype(F32)
        query_out[:, lanes] = total.astype(BF16)
        total = own[:, lanes]
        for ref in d_got:
            total = total + ref[t * rows : (t + 1) * rows, :].astype(F32)
        doc_out[:, lanes] = total.astype(BF16)
    losses = [chip_loss[...]] + [gather3(ref[tiles * rows :, :]) for ref in d_got]
    loss[...] = (tree_sum(losses) / all_pairs[:, :128])[:1]


def local(queries, documents, user_ids):
    rows, width = queries.shape
    quarters = lax.axis_size("quarter")
    plane = lax.axis_size("lane") * lax.axis_size("chip")
    devices = quarters * plane * 2
    batch_rows = float(devices * rows)
    scale = 3.0 / math.sqrt(width)
    cols = quarters * rows
    half = plane * rows
    piece = ((rows, width), BF16)

    d_parts = send_pieces([documents] * plane, PLANE)
    q_parts = send_pieces([queries] * quarters, "quarter")

    counts, total, positive, q_own, d_own = call(
        functools.partial(id_kernel, rows, plane),
        [((1, cols), F32), ((8, cols), F32), ((2 * half, rows), F32), piece, piece],
        user_ids.reshape(quarters * plane, 2 * rows),
        queries,
        documents,
        scratch=[
            pltpu.VMEM((quarters * plane, 2 * rows), F32),
            pltpu.VMEM((quarters * plane, 2 * rows), user_ids.dtype),
            pltpu.SemaphoreType.DMA((3,)),
        ],
        in_hbm=True,
    )
    d_parts[0], q_parts[0] = d_own, q_own
    d_parts = [d_parts[k] for k in piece_order(plane)]
    d_first = jnp.concatenate(d_parts[:-1], 0)
    first_other = swap_cores(d_first)
    last_other = swap_cores(d_parts[-1])
    q_mine = jnp.concatenate(q_parts, 0)
    docs = jnp.concatenate([d_first, d_parts[-1], first_other, last_other], 0)

    scores, stats = call(
        functools.partial(score_kernel, scale, rows),
        [((2 * half, cols), F32), ((8, cols), F32)],
        docs,
        q_mine,
        positive,
    )
    stats_all = send_pieces([stats] * quarters, "quarter")
    q_other = swap_cores(q_mine)
    shares = call(functools.partial(share_kernel, scale, rows), [piece] * (quarters - 1), scores, stats, docs)
    q_got = send_pieces([None] + list(shares), "quarter")

    w_mine, w_send, gains, line_loss = call(
        functools.partial(weight_kernel, batch_rows, rows),
        [((half, cols), BF16), ((half + 8, cols), BF16), ((rows, 8), F32), ((8, 128), F32)],
        scores,
        *stats_all,
        counts,
        total,
        positive,
    )
    w_in = swap_cores(w_send)
    (own_query,) = call(functools.partial(own_kernel, scale), [((rows, width), F32)], w_mine, w_send, docs)
    own_doc, chip_loss, *d_share = call(
        functools.partial(doc_kernel, scale, rows),
        [((rows, width), F32), ((8, 128), F32)] + [((rows * width // LANES + 8, LANES), BF16)] * (plane - 1),
        w_mine,
        w_in,
        q_mine,
        q_other,
        line_loss,
    )
    d_got = send_pieces([d_share[0]] + list(d_share), PLANE)
    query_grad, doc_grad, loss = call(
        functools.partial(sum_kernel, quarters - 1),
        [piece, piece, ((1, 128), F32)],
        own_query,
        gains,
        own_doc,
        chip_loss,
        total,
        *q_got[1:],
        *d_got[1:],
    )
    return query_grad, doc_grad, loss[0, 0]


def solution(mesh):
    wide, narrow = mesh.shape["wide"], mesh.shape["narrow"]
    grid = Mesh(mesh.devices.reshape(QUARTERS, wide // QUARTERS, narrow // 2, 2), ALL)

    return jax.shard_map(
        local,
        mesh=grid,
        in_specs=(P(ALL, None), P(ALL, None), P()),
        out_specs=(P(ALL, None), P(ALL, None), P()),
        check_vma=False,
    )
```

```python
import functools
import math

import jax
import jax.numpy as jnp
from jax import lax
from jax.experimental import pallas as pl
from jax.experimental.pallas import tpu as pltpu
from jax.sharding import Mesh, PartitionSpec as P


QUARTERS = 4
ALL = ("quarter", "lane", "chip", "core")
PLANE = ("lane", "chip")
DIRECT = 8
CHUNK = 256
LANES = 128
F32, BF16 = jnp.float32, jnp.bfloat16


def send_pieces(pieces, axes):
    count = len(pieces)
    if count <= DIRECT:
        out = [pieces[0]] + [None] * (count - 1)
        for k in range(count - 1, 0, -1):
            out[k] = lax.ppermute(pieces[k], axes, [(i, i ^ k) for i in range(count)])
        return out
    order = jnp.bitwise_xor(lax.axis_index(axes), jnp.arange(count))
    placed = jnp.take(jnp.stack(pieces), order, axis=0)
    moved = jnp.take(lax.all_to_all(placed, axes, 0, 0, tiled=True), order, axis=0)
    return [pieces[0]] + [moved[k] for k in range(1, count)]


def swap_cores(array):
    return lax.ppermute(array, "core", [(0, 1), (1, 0)])


def tree_sum(terms):
    while len(terms) > 1:
        terms = [terms[i] + terms[i + 1] for i in range(0, len(terms), 2)]
    return terms[0]


def contract(a, b, da, db):
    return lax.dot_general(a, b, (((da,), (db,)), ((), ())), preferred_element_type=F32)


def piece_order(plane):
    return [0] + list(range(plane - 1, 0, -1))


def call(kernel, outs, *args, scratch=(), in_hbm=False):
    vmem = pl.BlockSpec(memory_space=pltpu.VMEM)
    sizes = [a.size * a.dtype.itemsize for a in args]
    sizes += [math.prod(shape) * jnp.dtype(dtype).itemsize for shape, dtype in outs]
    return pl.pallas_call(
        kernel,
        out_shape=[jax.ShapeDtypeStruct(shape, dtype) for shape, dtype in outs],
        in_specs=[pl.BlockSpec(memory_space=pl.ANY) if in_hbm else vmem] * len(args),
        out_specs=[vmem] * len(outs),
        scratch_shapes=list(scratch),
        compiler_params=pltpu.CompilerParams(vmem_limit_bytes=min(3 * sum(sizes), 40 << 20) + (6 << 20)),
    )(*args)


def spread(line, width):
    lane = lax.broadcasted_iota(jnp.int32, (8, width), 1)
    parts = [jnp.broadcast_to(part.astype(F32)[:, :1], (8, width)) for part in split3(line)]
    value = jnp.where(lane == 0, parts[0], jnp.where(lane == 1, parts[1], jnp.where(lane == 2, parts[2], 0.0)))
    return value.astype(BF16)


def gather3(rows):
    parts = [rows[:, i : i + 1] for i in range(3)]
    return jnp.broadcast_to(join3(*parts), (8, 128))


def each_chunk(total, body):
    if total <= 2 * CHUNK:
        for i in range(total // CHUNK):
            body(i * CHUNK)
    else:

        @pl.loop(0, total // CHUNK)
        def _(i):
            body(pl.multiple_of(i * CHUNK, CHUNK))


def halves(row, core, rows):
    low, high = row[:, :rows], row[:, rows:]
    return jnp.where(core == 0, low, high), jnp.where(core == 0, high, low)


def id_kernel(rows, plane, ids_in, queries, documents, counts, total, positive, q_own, d_own, found, ids, sems):
    quarters = ids.shape[0] // plane
    my_quarter, my_core = lax.axis_index("quarter"), lax.axis_index("core")
    my_plane = lax.axis_index(PLANE)
    copies = [
        pltpu.make_async_copy(src, dst, sems.at[i])
        for i, (src, dst) in enumerate(((ids_in, ids), (documents, d_own), (queries, q_own)))
    ]
    for copy in copies:
        copy.start()
    copies[0].wait()
    chips, lanes = ids.shape
    square = ids[...]
    if chips < lanes:
        square = jnp.concatenate([square, jnp.zeros((lanes - chips, lanes), square.dtype)], 0)
    tall = jnp.transpose(square)
    for z in range(quarters):

        def count(chip):
            row = ids[pl.ds(chip, 1), :]
            same = jnp.zeros((lanes, lanes), F32)
            for other in range(z * plane, (z + 1) * plane):
                same += (tall[:, other : other + 1] == row).astype(F32)
            found[pl.ds(chip, 1), :] = jnp.sum(same, 0, keepdims=True)

        if plane <= DIRECT:
            for chip in range(z * plane, (z + 1) * plane):
                count(chip)
        else:
            pl.loop(z * plane, (z + 1) * plane)(count)
    total[...] = jnp.broadcast_to(jnp.sum(jnp.sum(found[...], 0, keepdims=True), 1, keepdims=True), total.shape)
    for k in range(quarters):
        row = found[pl.ds((my_quarter ^ k) * plane + my_plane, 1), :]
        counts[:, k * rows : (k + 1) * rows] = halves(row, my_core, rows)[0]
    own = halves(ids[pl.ds(my_quarter * plane + my_plane, 1), :], my_core, rows)[0]
    for k, piece in enumerate(piece_order(plane)):
        row = ids[pl.ds(my_quarter * plane + (my_plane ^ piece), 1), :]
        column = jnp.transpose(jnp.broadcast_to(row, (8, lanes)))[:, :1]
        low, high = (column[:rows] == own).astype(F32), (column[rows:] == own).astype(F32)
        positive[k * rows : (k + 1) * rows, :] = jnp.where(my_core == 0, low, high)
        positive[(plane + k) * rows : (plane + k + 1) * rows, :] = jnp.where(my_core == 0, high, low)
    for copy in copies[1:]:
        copy.wait()


def split3(x):
    high = x.astype(BF16)
    rest = x - high.astype(F32)
    middle = rest.astype(BF16)
    return high, middle, (rest - middle.astype(F32)).astype(BF16)


def join3(high, middle, low):
    return (high.astype(F32) + middle.astype(F32)) + low.astype(F32)


def score_kernel(scale, rows, docs, queries, positive, scores, stats, run):
    count = docs.shape[0]
    cols = queries.shape[0]
    run[...] = jnp.zeros(run.shape, F32)
    run[0:1, :] = jnp.full((1, cols), -jnp.inf, F32)
    queries_now = queries[...]

    def first(at):
        part = contract(docs[pl.ds(at, CHUNK), :], queries_now, 1, 1) * scale
        scores[pl.ds(at, CHUNK), :] = part
        run[0:1, :] = jnp.maximum(run[0:1, :], jnp.max(part, 0, keepdims=True))
        chosen = jnp.where(positive[pl.ds(at, CHUNK), :] > 0.0, part[:, :rows], 0.0)
        run[1:2, :rows] += jnp.sum(chosen, 0, keepdims=True)

    each_chunk(count, first)
    peak = run[0:1, :]

    def second(at):
        run[2:3, :] += jnp.sum(jnp.exp(scores[pl.ds(at, CHUNK), :] - peak), 0, keepdims=True)

    each_chunk(count, second)
    stats[:, :cols] = peak + jnp.log(run[2:3, :])
    stats[:, cols:] = jnp.broadcast_to(jnp.sum(run[1:2, :rows], 1, keepdims=True), (1, LANES))


def share_kernel(scale, rows, scores, stats, docs, *outs):
    cols = scores.shape[1]
    lse = stats[0:1, :cols]
    total = None
    for at in range(0, scores.shape[0], 2 * CHUNK):
        probs = jnp.exp(scores[at : at + 2 * CHUNK, :] - lse)
        part = contract(jnp.transpose(probs)[rows:].astype(BF16), docs[at : at + 2 * CHUNK, :], 1, 0)
        total = part if total is None else total + part
    total = (total * scale).astype(BF16)
    for k, out in enumerate(outs):
        out[...] = total[k * rows : (k + 1) * rows]


def weight_kernel(batch_rows, rows, scores, s0, s1, s2, s3, counts, total, positive, *outs):
    w_mine, w_send, gains, loss = outs
    tail = w_mine.shape[0]
    cols = scores.shape[1]
    half = scores.shape[0] // 2
    stats = [s[...] for s in (s0, s1, s2, s3)]
    rest = cols // rows
    lses = [
        jnp.concatenate([s[0:1, (k ^ j) * rows : (k ^ j) * rows + rows] for k in range(rest)], 1)
        for j, s in enumerate(stats)
    ]
    top = functools.reduce(jnp.maximum, lses)
    log_denom = top + jnp.log(tree_sum([jnp.exp(a - top) for a in lses]))
    row_counts = counts[...]
    per_pair = batch_rows / total[:1, :]

    def fill(out, base):
        def body(at):
            src = pl.ds(base + at, CHUNK)
            raw = row_counts * jnp.exp(scores[src, :] - log_denom)
            own = raw[:, : 2 * rows]
            pad = jnp.concatenate([positive[src, :], jnp.zeros((CHUNK, rows), F32)], 1)
            raw = jnp.concatenate([own - pad, raw[:, 2 * rows :]], 1)
            out[pl.ds(at, CHUNK), :] = (raw * per_pair).astype(BF16)

        each_chunk(half, body)

    fill(w_send, half)
    fill(w_mine, 0)
    factor = row_counts[:, :rows] * per_pair[:, :rows]
    lanes = [factor * jnp.exp(a[:, :rows] - log_denom[:, :rows]) for a in lses]
    tall = jnp.concatenate(lanes + lanes, 0)
    gains[...] = jnp.transpose(jnp.concatenate([tall, tall], 1))[:rows]
    terms = row_counts * log_denom
    line = tree_sum(
        [
            jnp.sum(terms[:, k * rows : (k + 1) * rows], 1, keepdims=True) - stats[k][:, cols : cols + 1]
            for k in range(rest)
        ]
    )
    line = jnp.broadcast_to(line, loss.shape)
    loss[...] = line
    w_send[tail:, :] = spread(line, w_send.shape[1])


def own_kernel(scale, w_mine, w_send, docs, out):
    half = w_mine.shape[0]
    rows = out.shape[0]
    total = None
    for base, ref in ((0, w_mine), (half, w_send)):
        for at in range(0, half, CHUNK):
            w = jnp.transpose(ref[at : at + CHUNK, :128].astype(F32))[:rows].astype(BF16)
            part = contract(w, docs[base + at : base + at + CHUNK, :], 1, 0)
            total = part if total is None else total + part
    out[...] = total * scale


def doc_kernel(scale, rows, w_mine, w_in, q_mine, q_other, loss, own, chip_loss, *outs):
    half = w_mine.shape[0]
    line = loss[...] + gather3(w_in[half:, :])
    chip_loss[...] = line
    tiles = own.shape[1] // LANES
    note = spread(line, LANES)
    order = piece_order(half // rows)
    for out in outs:
        out[tiles * rows :, :] = note
    for at in range(0, half, CHUNK):
        part = contract(w_mine[at : at + CHUNK, :], q_mine[...], 1, 0)
        part = (part + contract(w_in[at : at + CHUNK, :], q_other[...], 1, 0)) * scale
        for j in range(at // rows, (at + CHUNK) // rows):
            share = part[j * rows - at : (j + 1) * rows - at]
            k = order[j]
            if k == 0:
                own[...] = share
            else:
                for t in range(tiles):
                    outs[k - 1][t * rows : (t + 1) * rows, :] = share[:, t * LANES : (t + 1) * LANES].astype(BF16)


def sum_kernel(peers, own_query, gains, own, chip_loss, all_pairs, *refs):
    *got, query_out, doc_out, loss = refs
    q_got, d_got = got[:peers], got[peers:]
    rows = own.shape[0]
    tiles = own.shape[1] // LANES
    gain = [gains[:, k : k + 1] for k in range(peers + 1)]
    for t in range(tiles):
        lanes = slice(t * LANES, (t + 1) * LANES)
        total = own_query[:, lanes]
        for k, ref in enumerate(q_got, 1):
            total = total + gain[k] * ref[:, lanes].astype(F32)
        query_out[:, lanes] = total.astype(BF16)
        total = own[:, lanes]
        for ref in d_got:
            total = total + ref[t * rows : (t + 1) * rows, :].astype(F32)
        doc_out[:, lanes] = total.astype(BF16)
    losses = [chip_loss[...]] + [gather3(ref[tiles * rows :, :]) for ref in d_got]
    loss[...] = (tree_sum(losses) / all_pairs[:, :128])[:1]


def local(queries, documents, user_ids):
    rows, width = queries.shape
    quarters = lax.axis_size("quarter")
    plane = lax.axis_size("lane") * lax.axis_size("chip")
    devices = quarters * plane * 2
    batch_rows = float(devices * rows)
    scale = 3.0 / math.sqrt(width)
    cols = quarters * rows
    half = plane * rows
    piece = ((rows, width), BF16)

    d_parts = send_pieces([documents] * plane, PLANE)
    q_parts = send_pieces([queries] * quarters, "quarter")

    counts, total, positive, q_own, d_own = call(
        functools.partial(id_kernel, rows, plane),
        [((1, cols), F32), ((8, cols), F32), ((2 * half, rows), F32), piece, piece],
        user_ids.reshape(quarters * plane, 2 * rows),
        queries,
        documents,
        scratch=[
            pltpu.VMEM((quarters * plane, 2 * rows), F32),
            pltpu.VMEM((quarters * plane, 2 * rows), user_ids.dtype),
            pltpu.SemaphoreType.DMA((3,)),
        ],
        in_hbm=True,
    )
    d_parts[0], q_parts[0] = d_own, q_own
    d_parts = [d_parts[k] for k in piece_order(plane)]
    d_first = jnp.concatenate(d_parts[:-1], 0)
    first_other = swap_cores(d_first)
    last_other = swap_cores(d_parts[-1])
    q_mine = jnp.concatenate(q_parts, 0)
    docs = jnp.concatenate([d_first, d_parts[-1], first_other, last_other], 0)

    scores, stats = call(
        functools.partial(score_kernel, scale, rows),
        [((2 * half, cols), F32), ((1, cols + LANES), F32)],
        docs,
        q_mine,
        positive,
        scratch=[pltpu.VMEM((8, cols), F32)],
    )
    stats_all = send_pieces([stats] * quarters, "quarter")
    q_other = swap_cores(q_mine)
    shares = call(functools.partial(share_kernel, scale, rows), [piece] * (quarters - 1), scores, stats, docs)
    q_got = send_pieces([None] + list(shares), "quarter")

    w_mine, w_send, gains, line_loss = call(
        functools.partial(weight_kernel, batch_rows, rows),
        [((half, cols), BF16), ((half + 8, cols), BF16), ((rows, 8), F32), ((8, 128), F32)],
        scores,
        *stats_all,
        counts,
        total,
        positive,
    )
    w_in = swap_cores(w_send)
    (own_query,) = call(functools.partial(own_kernel, scale), [((rows, width), F32)], w_mine, w_send, docs)
    own_doc, chip_loss, *d_share = call(
        functools.partial(doc_kernel, scale, rows),
        [((rows, width), F32), ((8, 128), F32)] + [((rows * width // LANES + 8, LANES), BF16)] * (plane - 1),
        w_mine,
        w_in,
        q_mine,
        q_other,
        line_loss,
    )
    d_got = send_pieces([d_share[0]] + list(d_share), PLANE)
    query_grad, doc_grad, loss = call(
        functools.partial(sum_kernel, quarters - 1),
        [piece, piece, ((1, 128), F32)],
        own_query,
        gains,
        own_doc,
        chip_loss,
        total,
        *q_got[1:],
        *d_got[1:],
    )
    return query_grad, doc_grad, loss[0, 0]


def solution(mesh):
    wide, narrow = mesh.shape["wide"], mesh.shape["narrow"]
    grid = Mesh(mesh.devices.reshape(QUARTERS, wide // QUARTERS, narrow // 2, 2), ALL)

    return jax.shard_map(
        local,
        mesh=grid,
        in_specs=(P(ALL, None), P(ALL, None), P()),
        out_specs=(P(ALL, None), P(ALL, None), P()),
        check_vma=False,
    )
```

```python
import functools
import math

import jax
import jax.numpy as jnp
from jax import lax
from jax.experimental import pallas as pl
from jax.experimental.pallas import tpu as pltpu
from jax.sharding import Mesh, PartitionSpec as P


QUARTERS = 4
ALL = ("quarter", "lane", "chip", "core")
PLANE = ("lane", "chip")
DIRECT = 8
CHUNK = 256
LANES = 128
F32, BF16 = jnp.float32, jnp.bfloat16


def send_pieces(pieces, axes):
    count = len(pieces)
    if count <= DIRECT:
        out = [pieces[0]] + [None] * (count - 1)
        for k in range(count - 1, 0, -1):
            out[k] = lax.ppermute(pieces[k], axes, [(i, i ^ k) for i in range(count)])
        return out
    order = jnp.bitwise_xor(lax.axis_index(axes), jnp.arange(count))
    placed = jnp.take(jnp.stack(pieces), order, axis=0)
    moved = jnp.take(lax.all_to_all(placed, axes, 0, 0, tiled=True), order, axis=0)
    return [pieces[0]] + [moved[k] for k in range(1, count)]


def swap_cores(array):
    return lax.ppermute(array, "core", [(0, 1), (1, 0)])


def tree_sum(terms):
    while len(terms) > 1:
        terms = [terms[i] + terms[i + 1] for i in range(0, len(terms), 2)]
    return terms[0]


def contract(a, b, da, db):
    return lax.dot_general(a, b, (((da,), (db,)), ((), ())), preferred_element_type=F32)


def piece_order(plane):
    return [0] + list(range(plane - 1, 0, -1))


def call(kernel, outs, *args, scratch=(), in_hbm=False):
    vmem = pl.BlockSpec(memory_space=pltpu.VMEM)
    sizes = [a.size * a.dtype.itemsize for a in args]
    sizes += [math.prod(shape) * jnp.dtype(dtype).itemsize for shape, dtype in outs]
    return pl.pallas_call(
        kernel,
        out_shape=[jax.ShapeDtypeStruct(shape, dtype) for shape, dtype in outs],
        in_specs=[pl.BlockSpec(memory_space=pl.ANY) if in_hbm else vmem] * len(args),
        out_specs=[vmem] * len(outs),
        scratch_shapes=list(scratch),
        compiler_params=pltpu.CompilerParams(vmem_limit_bytes=min(3 * sum(sizes), 40 << 20) + (6 << 20)),
    )(*args)


def spread(line, width):
    lane = lax.broadcasted_iota(jnp.int32, (8, width), 1)
    parts = [jnp.broadcast_to(part.astype(F32)[:, :1], (8, width)) for part in split3(line)]
    value = jnp.where(lane == 0, parts[0], jnp.where(lane == 1, parts[1], jnp.where(lane == 2, parts[2], 0.0)))
    return value.astype(BF16)


def gather3(rows):
    parts = [rows[:, i : i + 1] for i in range(3)]
    return jnp.broadcast_to(join3(*parts), (8, 128))


def each_chunk(total, body):
    if total <= 2 * CHUNK:
        for i in range(total // CHUNK):
            body(i * CHUNK)
    else:

        @pl.loop(0, total // CHUNK)
        def _(i):
            body(pl.multiple_of(i * CHUNK, CHUNK))


def halves(row, core, rows):
    low, high = row[:, :rows], row[:, rows:]
    return jnp.where(core == 0, low, high), jnp.where(core == 0, high, low)


def id_kernel(rows, plane, ids_in, queries, documents, counts, total, positive, q_own, d_own, found, ids, sems):
    quarters = ids.shape[0] // plane
    my_quarter, my_core = lax.axis_index("quarter"), lax.axis_index("core")
    my_plane = lax.axis_index(PLANE)
    copies = [
        pltpu.make_async_copy(src, dst, sems.at[i])
        for i, (src, dst) in enumerate(((ids_in, ids), (documents, d_own), (queries, q_own)))
    ]
    for copy in copies:
        copy.start()
    copies[0].wait()
    chips, lanes = ids.shape
    square = ids[...]
    if chips < lanes:
        square = jnp.concatenate([square, jnp.zeros((lanes - chips, lanes), square.dtype)], 0)
    tall = jnp.transpose(square)
    for z in range(quarters):

        def count(chip):
            row = ids[pl.ds(chip, 1), :]
            same = jnp.zeros((lanes, lanes), F32)
            for other in range(z * plane, (z + 1) * plane):
                same += (tall[:, other : other + 1] == row).astype(F32)
            found[pl.ds(chip, 1), :] = jnp.sum(same, 0, keepdims=True)

        if plane <= DIRECT:
            for chip in range(z * plane, (z + 1) * plane):
                count(chip)
        else:
            pl.loop(z * plane, (z + 1) * plane)(count)
    total[...] = jnp.broadcast_to(jnp.sum(jnp.sum(found[...], 0, keepdims=True), 1, keepdims=True), total.shape)
    for k in range(quarters):
        row = found[pl.ds((my_quarter ^ k) * plane + my_plane, 1), :]
        counts[:, k * rows : (k + 1) * rows] = halves(row, my_core, rows)[0]
    own = halves(ids[pl.ds(my_quarter * plane + my_plane, 1), :], my_core, rows)[0]
    for k, piece in enumerate(piece_order(plane)):
        row = ids[pl.ds(my_quarter * plane + (my_plane ^ piece), 1), :]
        column = jnp.transpose(jnp.broadcast_to(row, (8, lanes)))[:, :1]
        low, high = (column[:rows] == own).astype(F32), (column[rows:] == own).astype(F32)
        positive[k * rows : (k + 1) * rows, :] = jnp.where(my_core == 0, low, high)
        positive[(plane + k) * rows : (plane + k + 1) * rows, :] = jnp.where(my_core == 0, high, low)
    for copy in copies[1:]:
        copy.wait()


def split3(x):
    high = x.astype(BF16)
    rest = x - high.astype(F32)
    middle = rest.astype(BF16)
    return high, middle, (rest - middle.astype(F32)).astype(BF16)


def join3(high, middle, low):
    return (high.astype(F32) + middle.astype(F32)) + low.astype(F32)


def score_kernel(scale, rows, docs, queries, positive, scores, stats, run):
    count = docs.shape[0]
    cols = queries.shape[0]
    run[...] = jnp.zeros(run.shape, F32)
    run[0:1, :] = jnp.full((1, cols), -jnp.inf, F32)
    queries_now = queries[...]

    def first(at):
        part = contract(docs[pl.ds(at, CHUNK), :], queries_now, 1, 1) * scale
        scores[pl.ds(at, CHUNK), :] = part
        run[0:1, :] = jnp.maximum(run[0:1, :], jnp.max(part, 0, keepdims=True))
        chosen = jnp.where(positive[pl.ds(at, CHUNK), :] > 0.0, part[:, :rows], 0.0)
        run[1:2, :rows] += jnp.sum(chosen, 0, keepdims=True)

    each_chunk(count, first)
    peak = run[0:1, :]

    def second(at):
        run[2:3, :] += jnp.sum(jnp.exp(scores[pl.ds(at, CHUNK), :] - peak), 0, keepdims=True)

    each_chunk(count, second)
    stats[:, :cols] = peak + jnp.log(run[2:3, :])
    stats[:, cols:] = jnp.broadcast_to(jnp.sum(run[1:2, :rows], 1, keepdims=True), (1, LANES))


def share_kernel(scale, rows, blocks, scores, stats, docs, *outs):
    low = min(blocks) // 2 * 2 * rows
    high = (max(blocks) // 2 + 1) * 2 * rows
    lse = stats[0:1, low:high]
    total = None
    for at in range(0, scores.shape[0], 2 * CHUNK):
        probs = jnp.transpose(jnp.exp(scores[at : at + 2 * CHUNK, low:high] - lse)).astype(BF16)
        probs = jnp.concatenate([probs[k * rows - low : (k + 1) * rows - low] for k in blocks], 0)
        part = contract(probs, docs[at : at + 2 * CHUNK, :], 1, 0)
        total = part if total is None else total + part
    total = (total * scale).astype(BF16)
    for i, out in enumerate(outs):
        out[...] = total[i * rows : (i + 1) * rows]


def weight_kernel(batch_rows, rows, scores, s0, s1, s2, s3, counts, total, positive, *outs):
    w_mine, w_send, gains, loss = outs
    tail = w_mine.shape[0]
    cols = scores.shape[1]
    half = scores.shape[0] // 2
    stats = [s[...] for s in (s0, s1, s2, s3)]
    rest = cols // rows
    lses = [
        jnp.concatenate([s[0:1, (k ^ j) * rows : (k ^ j) * rows + rows] for k in range(rest)], 1)
        for j, s in enumerate(stats)
    ]
    top = functools.reduce(jnp.maximum, lses)
    log_denom = top + jnp.log(tree_sum([jnp.exp(a - top) for a in lses]))
    row_counts = counts[...]
    per_pair = batch_rows / total[:1, :]

    def fill(out, base):
        def body(at):
            src = pl.ds(base + at, CHUNK)
            raw = row_counts * jnp.exp(scores[src, :] - log_denom)
            own = raw[:, : 2 * rows]
            pad = jnp.concatenate([positive[src, :], jnp.zeros((CHUNK, rows), F32)], 1)
            raw = jnp.concatenate([own - pad, raw[:, 2 * rows :]], 1)
            out[pl.ds(at, CHUNK), :] = (raw * per_pair).astype(BF16)

        each_chunk(half, body)

    fill(w_send, half)
    fill(w_mine, 0)
    factor = row_counts[:, :rows] * per_pair[:, :rows]
    lanes = [factor * jnp.exp(a[:, :rows] - log_denom[:, :rows]) for a in lses]
    tall = jnp.concatenate(lanes + lanes, 0)
    gains[...] = jnp.transpose(jnp.concatenate([tall, tall], 1))[:rows]
    terms = row_counts * log_denom
    line = tree_sum(
        [
            jnp.sum(terms[:, k * rows : (k + 1) * rows], 1, keepdims=True) - stats[k][:, cols : cols + 1]
            for k in range(rest)
        ]
    )
    line = jnp.broadcast_to(line, loss.shape)
    loss[...] = line
    w_send[tail:, :] = spread(line, w_send.shape[1])


def own_kernel(scale, w_mine, w_send, docs, out):
    half = w_mine.shape[0]
    rows = out.shape[0]
    total = None
    for base, ref in ((0, w_mine), (half, w_send)):
        for at in range(0, half, CHUNK):
            w = jnp.transpose(ref[at : at + CHUNK, :128].astype(F32))[:rows].astype(BF16)
            part = contract(w, docs[base + at : base + at + CHUNK, :], 1, 0)
            total = part if total is None else total + part
    out[...] = total * scale


def doc_kernel(scale, rows, w_mine, w_in, q_mine, q_other, loss, own, chip_loss, *outs):
    half = w_mine.shape[0]
    line = loss[...] + gather3(w_in[half:, :])
    chip_loss[...] = line
    tiles = own.shape[1] // LANES
    note = spread(line, LANES)
    order = piece_order(half // rows)
    for out in outs:
        out[tiles * rows :, :] = note
    for at in range(0, half, CHUNK):
        part = contract(w_mine[at : at + CHUNK, :], q_mine[...], 1, 0)
        part = (part + contract(w_in[at : at + CHUNK, :], q_other[...], 1, 0)) * scale
        for j in range(at // rows, (at + CHUNK) // rows):
            share = part[j * rows - at : (j + 1) * rows - at]
            k = order[j]
            if k == 0:
                own[...] = share
            else:
                for t in range(tiles):
                    outs[k - 1][t * rows : (t + 1) * rows, :] = share[:, t * LANES : (t + 1) * LANES].astype(BF16)


def sum_kernel(peers, own_query, gains, own, chip_loss, all_pairs, *refs):
    *got, query_out, doc_out, loss = refs
    q_got, d_got = got[:peers], got[peers:]
    rows = own.shape[0]
    tiles = own.shape[1] // LANES
    gain = [gains[:, k : k + 1] for k in range(peers + 1)]
    for t in range(tiles):
        lanes = slice(t * LANES, (t + 1) * LANES)
        total = own_query[:, lanes]
        for k, ref in enumerate(q_got, 1):
            total = total + gain[k] * ref[:, lanes].astype(F32)
        query_out[:, lanes] = total.astype(BF16)
        total = own[:, lanes]
        for ref in d_got:
            total = total + ref[t * rows : (t + 1) * rows, :].astype(F32)
        doc_out[:, lanes] = total.astype(BF16)
    losses = [chip_loss[...]] + [gather3(ref[tiles * rows :, :]) for ref in d_got]
    loss[...] = (tree_sum(losses) / all_pairs[:, :128])[:1]


def local(queries, documents, user_ids):
    rows, width = queries.shape
    quarters = lax.axis_size("quarter")
    plane = lax.axis_size("lane") * lax.axis_size("chip")
    devices = quarters * plane * 2
    batch_rows = float(devices * rows)
    scale = 3.0 / math.sqrt(width)
    cols = quarters * rows
    half = plane * rows
    piece = ((rows, width), BF16)

    d_parts = send_pieces([documents] * plane, PLANE)
    q_parts = send_pieces([queries] * quarters, "quarter")

    counts, total, positive, q_own, d_own = call(
        functools.partial(id_kernel, rows, plane),
        [((1, cols), F32), ((8, cols), F32), ((2 * half, rows), F32), piece, piece],
        user_ids.reshape(quarters * plane, 2 * rows),
        queries,
        documents,
        scratch=[
            pltpu.VMEM((quarters * plane, 2 * rows), F32),
            pltpu.VMEM((quarters * plane, 2 * rows), user_ids.dtype),
            pltpu.SemaphoreType.DMA((3,)),
        ],
        in_hbm=True,
    )
    d_parts[0], q_parts[0] = d_own, q_own
    d_parts = [d_parts[k] for k in piece_order(plane)]
    d_first = jnp.concatenate(d_parts[:-1], 0)
    first_other = swap_cores(d_first)
    last_other = swap_cores(d_parts[-1])
    q_mine = jnp.concatenate(q_parts, 0)
    docs = jnp.concatenate([d_first, d_parts[-1], first_other, last_other], 0)

    scores, stats = call(
        functools.partial(score_kernel, scale, rows),
        [((2 * half, cols), F32), ((1, cols + LANES), F32)],
        docs,
        q_mine,
        positive,
        scratch=[pltpu.VMEM((8, cols), F32)],
    )
    stats_all = send_pieces([stats] * quarters, "quarter")
    q_other = swap_cores(q_mine)
    shares = [None] * quarters
    for blocks in ((2,), tuple(k for k in range(1, quarters) if k != 2)):
        outs = call(functools.partial(share_kernel, scale, rows, blocks), [piece] * len(blocks), scores, stats, docs)
        for k, out in zip(blocks, outs):
            shares[k] = out
    q_got = send_pieces(shares, "quarter")

    w_mine, w_send, gains, line_loss = call(
        functools.partial(weight_kernel, batch_rows, rows),
        [((half, cols), BF16), ((half + 8, cols), BF16), ((rows, 8), F32), ((8, 128), F32)],
        scores,
        *stats_all,
        counts,
        total,
        positive,
    )
    w_in = swap_cores(w_send)
    (own_query,) = call(functools.partial(own_kernel, scale), [((rows, width), F32)], w_mine, w_send, docs)
    own_doc, chip_loss, *d_share = call(
        functools.partial(doc_kernel, scale, rows),
        [((rows, width), F32), ((8, 128), F32)] + [((rows * width // LANES + 8, LANES), BF16)] * (plane - 1),
        w_mine,
        w_in,
        q_mine,
        q_other,
        line_loss,
    )
    d_got = send_pieces([d_share[0]] + list(d_share), PLANE)
    query_grad, doc_grad, loss = call(
        functools.partial(sum_kernel, quarters - 1),
        [piece, piece, ((1, 128), F32)],
        own_query,
        gains,
        own_doc,
        chip_loss,
        total,
        *q_got[1:],
        *d_got[1:],
    )
    return query_grad, doc_grad, loss[0, 0]


def solution(mesh):
    wide, narrow = mesh.shape["wide"], mesh.shape["narrow"]
    grid = Mesh(mesh.devices.reshape(QUARTERS, wide // QUARTERS, narrow // 2, 2), ALL)

    return jax.shard_map(
        local,
        mesh=grid,
        in_specs=(P(ALL, None), P(ALL, None), P()),
        out_specs=(P(ALL, None), P(ALL, None), P()),
        check_vma=False,
    )
```
